32 devices in a mesh: leaf: 32 (over z, y, x, core).
Axes of the slice: x: 2, y: 2, z: 4, core: 2. Of those that a mesh axis runs over, the one named last changes fastest.
Arguments:
- panels: bfloat16 [64, 64, 256], P('leaf'), may hold values from -6 to 6
- basis: bfloat16 [64, 64, 256], P('leaf'), may hold values from -0.375 to 0.375
- transfer: bfloat16 [64, 64, 64], P('leaf'), may hold values from -0.25 to 0.25
- near_blocks: bfloat16 [64, 27, 256, 256], P('leaf'), may hold values from -0.078125 to 0.078125
- coupling: bfloat16 [2, 343, 4096], replicated, may hold values from -0.0546875 to 0.0546875
- near_list: int32 [64, 27], P('leaf'), may hold values from -1 to 63, as said below
Outputs:
- product: bfloat16 [64, 64, 256], P('leaf')
The draws below stay inside these ranges and needn't reach their ends.
Inputs may be any that keep to these rules, and one draw needn't show every extreme that they name: `near_list`: row i lists, in an order of no meaning, leaf i and the leaves whose grid positions differ from it by at most one in each coordinate; -1 fills the other slots.
All inputs are finite; a program needn't handle non-finite values.
Results may differ from the reference program's by a relative error of at most 0.0035.
Values may be sent and summed in bfloat16 or wider, within the bound.
A program may use at most 192 MiB of HBM per device.

```python
import jax
import jax.numpy as jnp
from jax import lax

LEAF = 256
RANK = 64
COLS = 64
NNEAR = 27
SHIFTS = 343
LEAVES = 64
CLUSTERS = 8


def decode_drawn(indices, bit_count):
    coords = [jnp.zeros_like(indices) for a in range(3)]
    for k in range(bit_count):
        coords[k % 3] = coords[k % 3] + ((indices >> k & 1) << k // 3)
    return coords


def encode_drawn(coords, bit_count):
    result = jnp.zeros_like(coords[0])
    for k in range(bit_count):
        result = result + ((coords[k % 3] >> k // 3 & 1) << k)
    return result


def grid_extent_drawn(bit_count):
    return [2 ** len([k for k in range(bit_count) if k % 3 == a]) for a in range(3)]


def shuffle_rows(key, table, width):
    column = jnp.arange(table.shape[1], dtype=jnp.int32)[None, :]
    noise = jax.random.randint(key, table.shape, 0, 1 << 20, dtype=jnp.int32)
    score = jnp.where(table >= 0, 1 << 29, 0) + noise * 256 + column
    order = jnp.argsort(-score, axis=1)
    return jnp.take_along_axis(table, order, axis=1)[:, :width].astype(jnp.int32)


def near_rows(key, bit_count):
    count = 2 ** bit_count
    coords = decode_drawn(jnp.arange(count, dtype=jnp.int32), bit_count)
    extent = grid_extent_drawn(bit_count)
    entries = []
    for delta in [(a, b, c) for a in (-1, 0, 1) for b in (-1, 0, 1) for c in (-1, 0, 1)]:
        moved = [coords[a] + delta[a] for a in range(3)]
        inside = (moved[0] >= 0) & (moved[0] < extent[0]) & (moved[1] >= 0) & (moved[1] < extent[1]) & (moved[2] >= 0) & (moved[2] < extent[2])
        entries.append(jnp.where(inside, encode_drawn(moved, bit_count), -1))
    return shuffle_rows(key, jnp.stack(entries, axis=1), NNEAR)


def draw_near_list(key, part):
    return near_rows(jax.random.fold_in(key, 11), int(LEAVES).bit_length() - 1)


def levels(rng, shape, cuts, smallest, largest):
    level = 1.0
    for dim, shards_of in cuts:
        heights = jax.random.uniform(jax.random.fold_in(jax.random.fold_in(rng, 6), dim), (shards_of,), jnp.float32, smallest / len(cuts), largest / len(cuts))
        level = level * jnp.repeat(jnp.exp(heights), shape[dim] // shards_of).reshape((-1,) + (1,) * (len(shape) - 1 - dim))
    return level


def centred(stream_key, shape, spread, bound, split=(), kind=jnp.bfloat16):
    loudness = levels(stream_key, shape, split, -0.22, 0.18) if split else 1.0
    values = jax.random.normal(stream_key, shape, jnp.float32) * spread * loudness
    return jnp.minimum(jnp.maximum(values, -bound), bound).astype(kind)


def setup_inputs(seed: int = 0) -> dict:
    streams_of = jax.random.split(jax.random.key(seed), 7)
    return {
        "panels": centred(streams_of[0], (LEAVES, COLS, LEAF), 1.0, 6.0, ((0, 32),)),
        "basis": centred(streams_of[1], (LEAVES, RANK, LEAF), LEAF ** -0.5, 0.375, ((0, 32),)),
        "transfer": centred(streams_of[2], (LEAVES, RANK, RANK), (8 * RANK) ** -0.5, 0.25, ((0, 32),)),
        "near_blocks": centred(streams_of[3], (LEAVES, NNEAR, LEAF, LEAF), (NNEAR * LEAF) ** -0.5, 0.078125, ((0, 32),)),
        "coupling": centred(streams_of[4], (2, SHIFTS, RANK * RANK), (189 * RANK) ** -0.5, 0.0546875),
        "near_list": draw_near_list(jax.random.fold_in(streams_of[6], 71), 0),
    }


def decode(indices, bit_count):
    coords = [jnp.zeros_like(indices) for a in range(3)]
    for k in range(bit_count):
        coords[k % 3] = coords[k % 3] + (((indices >> k) & 1) << (k // 3))
    return coords


def encode(coords, bit_count):
    result = jnp.zeros_like(coords[0])
    for k in range(bit_count):
        result = result + (((coords[k % 3] >> (k // 3)) & 1) << k)
    return result


def grid_extent(bit_count):
    return [2 ** len([k for k in range(bit_count) if k % 3 == a]) for a in range(3)]


def far_table(cells, bit_count):
    coords = decode(cells, bit_count)
    extent = grid_extent(bit_count)
    entries = []
    for delta in [(a, b, c) for a in (-1, 0, 1) for b in (-1, 0, 1) for c in (-1, 0, 1)]:
        upper = [(coords[a] >> 1) + delta[a] for a in range(3)]
        inside = (upper[0] >= 0) & (upper[0] < extent[0] // 2) & (upper[1] >= 0) & (upper[1] < extent[1] // 2) & (upper[2] >= 0) & (upper[2] < extent[2] // 2)
        for child in [(a, b, c) for a in (0, 1) for b in (0, 1) for c in (0, 1)]:
            moved = [2 * upper[a] + child[a] for a in range(3)]
            apart = (jnp.abs(moved[0] - coords[0]) > 1) | (jnp.abs(moved[1] - coords[1]) > 1) | (jnp.abs(moved[2] - coords[2]) > 1)
            entries.append(jnp.where(inside & apart, encode(moved, bit_count), -1))
    return jnp.stack(entries, axis=-1).astype(jnp.int32)


def shift_code(targets, sources, bit_count):
    safe = jnp.maximum(sources, 0)
    first = decode(targets, bit_count)
    second = decode(safe, bit_count)
    return (49 * (second[0] - first[0] + 3) + 7 * (second[1] - first[1] + 3) + (second[2] - first[2] + 3)).astype(jnp.int32)


def couple(coef_table, table, rows, codes):
    valid = (rows >= 0).astype(jnp.float32)
    picked = jnp.take(coef_table, jnp.maximum(rows, 0), axis=0).astype(jnp.float32) * valid[:, None, None]
    mats = jnp.take(table, codes, axis=0).astype(jnp.float32).reshape(rows.shape[0], RANK, RANK)
    return jnp.einsum('jcr,jrs->cs', picked, mats)


def reference(panels, basis, transfer, near_blocks, coupling, near_list):
    bit_count = int(LEAVES).bit_length() - 1
    leaf_coef = jnp.einsum('lcq,lrq->lcr', panels.astype(jnp.float32), basis.astype(jnp.float32)).astype(jnp.bfloat16)
    partial_value = jnp.einsum('lcr,lrs->lcs', leaf_coef.astype(jnp.float32), transfer.astype(jnp.float32))
    cluster_coef = partial_value.reshape(CLUSTERS, 8, COLS, RANK).sum(axis=1).astype(jnp.bfloat16)
    leaf_ids = jnp.arange(LEAVES, dtype=jnp.int32)
    cluster_ids = jnp.arange(CLUSTERS, dtype=jnp.int32)
    far_leaf = far_table(leaf_ids, bit_count)
    far_cluster = far_table(cluster_ids, bit_count - 3)
    codes_leaf = shift_code(leaf_ids[:, None], far_leaf, bit_count)
    codes_cluster = shift_code(cluster_ids[:, None], far_cluster, bit_count - 3)
    down_coef = lax.map(lambda item: couple(cluster_coef, coupling[1], item[0], item[1]), (far_cluster, codes_cluster)).astype(jnp.bfloat16)
    leaf_far = lax.map(lambda item: couple(leaf_coef, coupling[0], item[0], item[1]), (far_leaf, codes_leaf))
    parent_down = jnp.repeat(down_coef, 8, axis=0).astype(jnp.float32)
    far_coef = (leaf_far + jnp.einsum('lcs,lrs->lcr', parent_down, transfer.astype(jnp.float32))).astype(jnp.bfloat16)
    far_term = jnp.einsum('lcr,lrq->lcq', far_coef.astype(jnp.float32), basis.astype(jnp.float32))

    def near_one(item):
        rows, blocks = item
        valid = (rows >= 0).astype(jnp.float32)
        picked = jnp.take(panels, jnp.maximum(rows, 0), axis=0).astype(jnp.float32) * valid[:, None, None]
        return jnp.einsum('kcq,kqp->cp', picked, blocks.astype(jnp.float32))

    near = lax.map(near_one, (near_list, near_blocks))
    return (near + far_term).astype(jnp.bfloat16)
```

```python
import functools

import jax
import jax.numpy as jnp
from jax import lax
from jax.experimental import pallas as pl
from jax.experimental.pallas import tpu as pltpu
from jax.sharding import PartitionSpec as P

MESH = pl.DeviceIdType.MESH
F32 = jnp.float32
BF16 = jnp.bfloat16
REACH = 3
SPAN = 2 * REACH + 1
TN = (((0,), (0,)), ((), ()))
NT = (((1,), (1,)), ((), ()))
OFFSETS = [(a, b, c) for a in (-1, 0, 1) for b in (-1, 0, 1) for c in (-1, 0, 1)]


def axis_bits(first, bit_count):
    return [[b for b in range(bit_count) if (b + first) % 3 == a] for a in range(3)]


def coords_of(index, bits):
    return [
        sum(((index // 2**b) % 2) * 2**p for p, b in enumerate(bits[a])) + index * 0
        for a in range(3)
    ]


def index_of(coords, bits):
    return sum(((coords[a] // 2**p) % 2) * 2**b for a in range(3) for p, b in enumerate(bits[a]))


def inside(coords, bits):
    ok = None
    for a in range(3):
        here = (coords[a] >= 0) & (coords[a] < 2 ** len(bits[a]))
        ok = here if ok is None else ok & here
    return ok


def far_mats(targets, bit_count, coupling, level, spread, mats):
    half = coupling.shape[1] // 2
    count = 2 ** (bit_count - 3)

    @pl.loop(0, min(count, 27))
    def _(i):
        upper, _, ok = candidate(targets[0], bit_count, i)
        columns = []
        for l, target in enumerate(targets):
            column = []
            for h in range(8):
                d = [2 * upper[a] + (h >> a & 1) - target[a] for a in range(3)]
                apart = (jnp.abs(d[0]) > 1) | (jnp.abs(d[1]) > 1) | (jnp.abs(d[2]) > 1)
                use = ok & apart
                code = (SPAN * (d[0] + REACH) + d[1] + REACH) * SPAN + d[2] + REACH
                code = jnp.where(use, code, 0)
                at = (l * 8 + h) * 2 * half
                spread[at : at + 2 * half, :] = coupling[code].astype(F32)
                mat = spread[pl.ds(at + level, half, stride=2), :]
                mat = mat * jnp.where(use, 1.0, 0.0).astype(F32)
                column.append(mat.astype(BF16))
            columns.append(jnp.concatenate(column, axis=0))
        mats[i] = jnp.concatenate(columns, axis=1) if len(columns) > 1 else columns[0]


def candidate(target, bit_count, i):
    bits = axis_bits(0, bit_count - 3)
    home = [c // 2 for c in target]
    if 2 ** (bit_count - 3) <= 27:
        upper = coords_of(i, bits)
        ok = None
        for a in range(3):
            near = jnp.abs(upper[a] - home[a]) <= 1
            ok = near if ok is None else ok & near
        return upper, i, ok
    upper = [home[0] + i // 9 - 1, home[1] + (i // 3) % 3 - 1, home[2] + i % 3 - 1]
    ok = inside(upper, bits)
    return upper, jnp.where(ok, index_of([jnp.maximum(u, 0) for u in upper], bits), 0), ok


def far_sum(targets, bit_count, stacked, mats, rank):
    depth = 8 * rank // 2
    count = 2 ** (bit_count - 3)

    def step(i, total):
        _, q, _ = candidate(targets[0], bit_count, i)
        rows = pl.ds(pl.multiple_of(q * depth, depth), depth)
        return total + lax.dot_general(stacked[rows, :], mats[i], TN, preferred_element_type=F32)

    start = jnp.zeros((2 * rank, 2 * rank * len(targets)), F32)
    total = lax.fori_loop(0, min(count, 27), step, start)
    result = []
    for l in range(len(targets)):
        part = total[:, 2 * rank * l : 2 * rank * (l + 1)]
        result.append(part[:rank, :rank] + part[rank:, rank:])
    return result


def kernel(
    n,
    panels,
    basis,
    transfer,
    blocks_hbm,
    coupling_hbm,
    near_list,
    out,
    all_panels,
    blocks,
    coupling,
    spread,
    mats0,
    mats1,
    coefs,
    parts,
    clusters,
    blocks_sem,
    coupling_sem,
    panel_send,
    panel_recv,
    coef_send,
    coef_recv,
    relay_send,
    relay_recv,
    part_send,
    part_recv,
    cluster_send,
    cluster_recv,
):
    leaf_dev, columns, points = panels.shape
    rank = basis.shape[1]
    slots = near_list.shape[1]
    half = rank // 2
    low_bits = leaf_dev.bit_length() - 1
    dev_bits = n.bit_length() - 1
    bit_count = low_bits + dev_bits
    group = 8 // leaf_dev
    groups = n // group
    chips = n // 2
    own_rows = leaf_dev * half
    me = lax.axis_index("leaf")
    chip, core = me // 2, me % 2
    mate = chip * 2 + 1 - core

    loads = [pltpu.make_async_copy(coupling_hbm, coupling, coupling_sem)]
    cut = slots // 3 if slots % 3 == 0 else slots
    for l in range(leaf_dev):
        for i in range(slots // cut):
            rows = pl.ds(i * cut, cut)
            loads.append(
                pltpu.make_async_copy(
                    blocks_hbm.at[l, rows],
                    blocks.at[l, rows],
                    blocks_sem.at[l * (slots // cut) + i],
                )
            )
    for load in loads:
        load.start()

    barrier = pltpu.get_barrier_semaphore()

    @pl.loop(1, n)
    def _(j):
        pl.semaphore_signal(
            barrier, inc=1, device_id=(lax.rem(me + j, n),), device_id_type=MESH
        )

    row = lax.broadcasted_iota(jnp.int32, (rank, rank), 0)
    col = lax.broadcasted_iota(jnp.int32, (rank, rank), 1)
    source = 2 * (row % half) + row // half
    order = jnp.where(col == source, 1.0, 0.0).astype(BF16)
    term = jnp.zeros((rank, columns), F32)
    for l in range(leaf_dev):
        flat = lax.dot_general(
            basis[l], panels[l], NT, preferred_element_type=F32
        ).astype(BF16)
        mixed = jnp.dot(order, flat, preferred_element_type=F32).astype(BF16)
        packed = jnp.concatenate([mixed[:half], mixed[half:]], axis=1)
        at = pl.multiple_of(me * own_rows, own_rows) + l * half
        coefs[pl.ds(pl.multiple_of(at, half), half), :] = packed
        sent = lax.dot_general(
            order, transfer[l], NT, preferred_element_type=F32
        ).astype(BF16)
        term = term + jnp.dot(sent, flat, preferred_element_type=F32)
    parts[0] = jnp.concatenate([term[:half], term[half:]], axis=1)
    for l in range(leaf_dev):
        all_panels[me * leaf_dev + l] = panels[l]

    mine = me // group
    parent = coords_of(mine, axis_bits(0, bit_count - 3))
    leaf_bits = axis_bits(0, bit_count)
    targets = [coords_of(me * leaf_dev + l, leaf_bits) for l in range(leaf_dev)]
    loads[0].wait()
    far_mats([parent], bit_count - 3, coupling, 1, spread, mats1)
    far_mats(targets, bit_count, coupling, 0, spread, mats0)

    pl.semaphore_wait(barrier, n - 1)

    def own_block(device):
        return coefs.at[pl.ds(pl.multiple_of(device * own_rows, own_rows), own_rows), :]

    places = min(4, chips)
    columns_of_chips = chips // places
    line, place = chip // places, lax.rem(chip, places)

    def coef_device(j, k):
        from_line = lax.rem(line - j + columns_of_chips, columns_of_chips)
        from_place = lax.rem(place - k + places, places)
        return (from_line * places + from_place) * 2 + core

    def coef_copy(j, k):
        to_line = lax.rem(line + j, columns_of_chips) if k is None else line
        to_place = place if k is None else lax.rem(place + k, places)
        m = j * places + (0 if k is None else k)
        block = own_block(me) if k is None else own_block(coef_device(j, 0))
        return pltpu.make_async_remote_copy(
            src_ref=block,
            dst_ref=block,
            send_sem=coef_send.at[m],
            recv_sem=coef_recv.at[m],
            device_id=((to_line * places + to_place) * 2 + core,),
            device_id_type=MESH,
        )

    def relay_copy(m, device):
        return pltpu.make_async_remote_copy(
            src_ref=own_block(device),
            dst_ref=own_block(device),
            send_sem=relay_send.at[m],
            recv_sem=relay_recv.at[m],
            device_id=(mate,),
            device_id_type=MESH,
        )

    def part_copy(j):
        base = (me // group) * group
        return pltpu.make_async_remote_copy(
            src_ref=parts.at[0],
            dst_ref=parts.at[j],
            send_sem=part_send.at[j],
            recv_sem=part_recv.at[j],
            device_id=(base + lax.rem(me - base + j, group),),
            device_id_type=MESH,
        )

    def cluster_block(p):
        return clusters.at[pl.ds(pl.multiple_of(p * half, half), half), :]

    def cluster_copy(j, p):
        return pltpu.make_async_remote_copy(
            src_ref=cluster_block(p),
            dst_ref=cluster_block(p),
            send_sem=cluster_send.at[j],
            recv_sem=cluster_recv.at[j],
            device_id=(lax.rem(me + j * group, n),),
            device_id_type=MESH,
        )

    bits = axis_bits(low_bits, dev_bits)
    where = coords_of(me, bits)

    def hop_of(o):
        x, y, z = OFFSETS[o]
        return (0, y, 0) if y else (x, 0, 0) if x else (0, 0, z)

    def moved(offset):
        there = [where[a] + offset[a] for a in range(3)]
        ok = inside(there, bits)
        return ok, jnp.where(ok, index_of([jnp.maximum(v, 0) for v in there], bits), 0)

    def panel_copy(o, source, receiver):
        first, count = 0, leaf_dev
        if leaf_dev == 2 and OFFSETS[o][0] != 0:
            first, count = (1 if OFFSETS[o][0] > 0 else 0), 1
        rows = pl.ds(source * leaf_dev + first, count)
        owned = hop_of(o) == OFFSETS[o]
        return pltpu.make_async_remote_copy(
            src_ref=panels.at[pl.ds(first, count)] if owned else all_panels.at[rows],
            dst_ref=all_panels.at[rows],
            send_sem=panel_send.at[o],
            recv_sem=panel_recv.at[o],
            device_id=(receiver,),
            device_id_type=MESH,
        )

    def sends(o, act):
        hop = hop_of(o)
        ok, to = moved(hop)
        known, source = moved([h - e for h, e in zip(hop, OFFSETS[o])])

        @pl.when(ok & known)
        def _():
            act(panel_copy(o, source, to))

    def receives(o):
        known, source = moved([-e for e in OFFSETS[o]])

        @pl.when(known)
        def _():
            panel_copy(o, source, me).wait_recv()

    reach = [o for o in range(27) if OFFSETS[o] != (0, 0, 0)]
    along_z = [o for o in reach if not OFFSETS[o][0] and not OFFSETS[o][1]]
    along_x = [o for o in reach if OFFSETS[o][0] and not OFFSETS[o][1]]
    along_y = [o for o in reach if OFFSETS[o][1]]

    def start(copy):
        copy.start()

    for j in range(1, group):
        part_copy(j).start()
    for o in along_z:
        sends(o, start)

    @pl.loop(1, columns_of_chips)
    def _(j):
        coef_copy(j, None).start()

    relay_copy(0, me).start()
    for k in range(1, places):
        coef_copy(0, k).start()
    for o in along_x + along_y:
        if hop_of(o) == OFFSETS[o]:
            sends(o, start)

    for j in range(1, group):
        part_copy(j).wait_recv()
    total = parts[0]
    for j in range(1, group):
        total = total + parts[j]
    clusters[pl.ds(pl.multiple_of(mine * half, half), half), :] = total.astype(BF16)

    for o in along_z:
        receives(o)
        for later in along_x + along_y:
            before = [e - h for e, h in zip(OFFSETS[later], hop_of(later))]
            if tuple(before) == OFFSETS[o]:
                sends(later, start)

    @pl.loop(1, columns_of_chips)
    def _(j):
        coef_copy(j, None).wait_recv()
        for k in range(1, places):
            coef_copy(j, k).start()
        relay_copy(j * places, coef_device(j, 0)).start()

    @pl.loop(1, groups)
    def _(j):
        cluster_copy(j, mine).start()

    for o in along_x:
        receives(o)
        for later in along_y:
            before = [e - h for e, h in zip(OFFSETS[later], hop_of(later))]
            if tuple(before) == OFFSETS[o]:
                sends(later, start)

    @pl.loop(0, columns_of_chips)
    def _(j):
        for k in range(1, places):
            coef_copy(j, k).wait_recv()
            relay_copy(j * places + k, coef_device(j, k)).start()

    @pl.loop(0, chips)
    def _(m):
        relay_copy(m, me).wait_recv()

    leaf_far = far_sum(targets, bit_count, coefs, mats0, rank)

    @pl.loop(1, groups)
    def _(j):
        cluster_copy(j, mine).wait_recv()

    down = far_sum([parent], bit_count - 3, clusters, mats1, rank)[0].astype(BF16)
    far_terms = []
    for l in range(leaf_dev):
        far = leaf_far[l] + lax.dot_general(down, transfer[l], NT, preferred_element_type=F32)
        far_terms.append(jnp.dot(far.astype(BF16), basis[l], preferred_element_type=F32))

    for o in along_y:
        receives(o)
    for load in loads[1:]:
        load.wait()
    for l in range(leaf_dev):
        total = far_terms[l]
        for k in range(slots):
            j = near_list[l, k]
            block = all_panels[jnp.maximum(j, 0)]
            block = jnp.where(j >= 0, block, jnp.zeros_like(block))
            total = total + jnp.dot(block, blocks[l, k], preferred_element_type=F32)
        out[l] = total.astype(BF16)

    for j in range(1, group):
        part_copy(j).wait_send()

    @pl.loop(0, chips)
    def _(m):
        relay_copy(m, me).wait_send()

    @pl.loop(1, columns_of_chips)
    def _(j):
        coef_copy(j, None).wait_send()

    @pl.loop(0, columns_of_chips)
    def _(j):
        for k in range(1, places):
            coef_copy(j, k).wait_send()

    @pl.loop(1, groups)
    def _(j):
        cluster_copy(j, mine).wait_send()

    for o in reach:
        sends(o, lambda copy: copy.wait_send())


def per_device(panels, basis, transfer, near_blocks, coupling, near_list):
    n = lax.axis_size("leaf")
    leaf_dev, columns, points = panels.shape
    rank = basis.shape[1]
    slots = near_list.shape[1]
    shifts = coupling.shape[1]
    half = rank // 2
    leaves = n * leaf_dev
    coupling = coupling.transpose(1, 0, 2).reshape(shifts, 2, half, 2 * rank)
    coupling = coupling.transpose(0, 2, 1, 3).reshape(shifts, rank, 2 * rank)
    group = 8 // leaf_dev
    vmem = pl.BlockSpec(memory_space=pltpu.VMEM)
    hbm = pl.BlockSpec(memory_space=pl.ANY)
    dma = pltpu.SemaphoreType.DMA
    return pl.pallas_call(
        functools.partial(kernel, n),
        out_shape=pltpu.VMEM(panels.shape, BF16),
        in_specs=[vmem, vmem, vmem, hbm, hbm, pl.BlockSpec(memory_space=pltpu.SMEM)],
        out_specs=vmem,
        scratch_shapes=[
            pltpu.VMEM((leaves, columns, points), BF16),
            pltpu.VMEM(near_blocks.shape, BF16),
            pltpu.VMEM(coupling.shape, BF16),
            pltpu.VMEM((leaf_dev * 8 * rank, 2 * rank), F32),
            pltpu.VMEM((min(leaves // 8, 27), 8 * half, 2 * rank * leaf_dev), BF16),
            pltpu.VMEM((min(leaves // 64, 27), 8 * half, 2 * rank), BF16),
            pltpu.VMEM((leaves * half, 2 * columns), BF16),
            pltpu.VMEM((group, half, 2 * columns), F32),
            pltpu.VMEM((n // group * half, 2 * columns), BF16),
            dma((leaf_dev * 3,)),
            dma,
            dma((27,)),
            dma((27,)),
            dma((n // 2,)),
            dma((n // 2,)),
            dma((n // 2,)),
            dma((n // 2,)),
            dma((group,)),
            dma((group,)),
            dma((n // group,)),
            dma((n // group,)),
        ],
        compiler_params=pltpu.CompilerParams(
            collective_id=0, has_side_effects=True, vmem_limit_bytes=60 * 2**20
        ),
    )(panels, basis, transfer, near_blocks, coupling, near_list)


def solution(mesh):
    placed = (
        P("leaf", None, None),
        P("leaf", None, None),
        P("leaf", None, None),
        P("leaf", None, None, None),
        P(),
        P("leaf", None),
    )
    return jax.shard_map(
        per_device, mesh=mesh, in_specs=placed, out_specs=P("leaf", None, None), check_vma=False
    )
```

```python
import functools

import jax
import jax.numpy as jnp
from jax import lax
from jax.experimental import pallas as pl
from jax.experimental.pallas import tpu as pltpu
from jax.sharding import PartitionSpec as P

MESH = pl.DeviceIdType.MESH
F32 = jnp.float32
BF16 = jnp.bfloat16
REACH = 3
SPAN = 2 * REACH + 1
TN = (((0,), (0,)), ((), ()))
NT = (((1,), (1,)), ((), ()))
COEFS, TERMS, CLUSTERS, SUMS = range(4)


def axis_bits(first, bit_count):
    return [[b for b in range(bit_count) if (b + first) % 3 == a] for a in range(3)]


def halved(index, times):
    return index // 2**times if isinstance(index, int) else lax.div(index, 2**times)


def bit_of(index, b):
    high = halved(index, b) if b else index
    return high % 2 if isinstance(index, int) else lax.rem(high, 2)


def coords_of(index, bits):
    return [
        sum(bit_of(index, b) * 2**p for p, b in enumerate(bits[a])) + index * 0 for a in range(3)
    ]


def index_of(coords, bits):
    return sum(bit_of(coords[a], p) * 2**b for a in range(3) for p, b in enumerate(bits[a]))


def inside(coords, bits):
    ok = None
    for a in range(3):
        here = (coords[a] >= 0) & (coords[a] < 2 ** len(bits[a]))
        ok = here if ok is None else ok & here
    return ok


def flipped(index, mask, bit_count):
    result = 0
    for b in range(bit_count):
        one, two = bit_of(index, b), bit_of(mask, b)
        result = result + (one + two - 2 * one * two) * 2**b
    return result


def extract(coupling, code, level, spread, at):
    half = coupling.shape[1] // 2
    spread[at : at + 2 * half, :] = coupling[code].astype(F32)
    return spread[pl.ds(at + level, half, stride=2), :].astype(BF16)


def code_of(d):
    return (SPAN * (d[0] + REACH) + d[1] + REACH) * SPAN + d[2] + REACH


def candidate(target, bit_count, i):
    bits = axis_bits(0, bit_count - 3)
    home = [c // 2 for c in target]
    if 2 ** (bit_count - 3) <= 27:
        upper = coords_of(i, bits)
        ok = None
        for a in range(3):
            near = jnp.abs(upper[a] - home[a]) <= 1
            ok = near if ok is None else ok & near
        return upper, i, ok
    upper = [home[0] + i // 9 - 1, home[1] + (i // 3) % 3 - 1, home[2] + i % 3 - 1]
    ok = inside(upper, bits)
    return upper, jnp.where(ok, index_of([jnp.maximum(u, 0) for u in upper], bits), 0), ok


def kernel(
    n,
    panels_hbm,
    basis_hbm,
    transfer_hbm,
    blocks_hbm,
    coupling_hbm,
    near_hbm,
    out,
    panels,
    basis,
    transfer,
    blocks,
    coupling,
    near_list,
    slot_of,
    spread,
    mats0,
    mats1,
    coefs,
    terms,
    clusters,
    kept,
    sent,
    sums,
    near,
    load_sem,
    panel_send,
    panel_recv,
    group_send,
    group_recv,
):
    leaf_dev, rank, points = basis.shape
    cols = panels.shape[1]
    slots = near_list.shape[1]
    shifts = coupling_hbm.shape[0]
    half = rank // 2
    low_bits = leaf_dev.bit_length() - 1
    dev_bits = n.bit_length() - 1
    bit_count = low_bits + dev_bits
    group = 8 // leaf_dev
    plane = min(8, n)
    plane_bits = plane.bit_length() - 1
    lines = n // plane
    teams = plane // group
    own_rows = leaf_dev * half
    me = lax.axis_index("leaf")
    line, spot = lax.div(me, plane), lax.rem(me, plane)

    loads = [
        pltpu.make_async_copy(source, target, load_sem.at[i])
        for i, (source, target) in enumerate(
            [
                (panels_hbm, panels.at[pl.ds(me * leaf_dev, leaf_dev)]),
                (basis_hbm, basis),
                (transfer_hbm, transfer),
                (near_hbm, near_list),
                (coupling_hbm, coupling.at[pl.ds(0, shifts)]),
                (blocks_hbm, blocks),
            ]
        )
    ]
    for load in loads[:5]:
        load.start()

    bits = axis_bits(low_bits, dev_bits)
    where = coords_of(me, bits)
    side = [1 - 2 * bit_of(c, 0) for c in where]
    kinds = [min(2 ** len(b), 3) for b in bits]

    def offset(a, kind):
        return side[a] * bit_of(kind, 0) - side[a] * halved(kind, 1)

    def moved(kind):
        there = [where[a] + offset(a, kind[a]) for a in range(3)]
        ok = inside(there, bits)
        return ok, jnp.where(ok, index_of([jnp.maximum(v, 0) for v in there], bits), me)

    def when(kind, ok, act):
        if all(k < 2 for k in kind):
            act()
        else:
            pl.when(ok)(act)

    def peer(r):
        return line * plane + flipped(spot, r, plane_bits)

    barrier = pltpu.get_barrier_semaphore()

    def greet(device):
        pl.semaphore_signal(barrier, inc=1, device_id=(device,), device_id_type=MESH)

    @pl.loop(1, lines)
    def _(j):
        greet(lax.rem(line + j, lines) * plane + spot)

    for r in range(1, plane):
        greet(peer(r))
    faces = [tuple(k if b == a else 0 for b in range(3)) for a in range(3) for k in range(1, kinds[a])]
    expected = lines - 1 + plane - 1
    for face in faces:
        ok, to = moved(face)
        when(face, ok, lambda: greet(to))
        expected = expected + jnp.where(ok, 1, 0)

    coupling[shifts] = jnp.zeros((rank, 2 * rank), BF16)

    for load in loads[:3]:
        load.wait()
    lane = lax.broadcasted_iota(jnp.int32, (half, 2 * cols), 1)

    def packed(value, at):
        spread[at : at + rank, :] = value
        even = spread[pl.ds(at, half, stride=2), :]
        odd = spread[pl.ds(at + 1, half, stride=2), :]
        return jnp.where(lane < cols, even, odd).astype(BF16)

    flats = []
    for l in range(leaf_dev):
        panel = panels[me * leaf_dev + l]
        flat = lax.dot_general(
            basis[l], jnp.concatenate([panel, panel], axis=0), NT, preferred_element_type=F32
        )
        at = pl.multiple_of(line * own_rows, own_rows) + l * half
        coefs[pl.ds(pl.multiple_of(at, half), half), :] = packed(flat, l * rank)
        flats.append(flat.astype(BF16))

    along_x, along_y, along_z = (range(1, k) for k in kinds)

    def search():
        loads[3].wait()

        @pl.loop(0, kinds[1] * kinds[2])
        def _(i):
            y, z = lax.div(i, kinds[2]), lax.rem(i, kinds[2])

            def find(l, leaf):
                total = 0
                for k in range(slots):
                    total = jnp.where(near_list[l, k] == leaf, k, total)
                return total

            _, device = moved((0, y, z))
            for l in range(leaf_dev):
                for m in range(leaf_dev):
                    slot_of[i, l * leaf_dev + m] = find(l, device * leaf_dev + m)
            for x in along_x:
                e = offset(0, x)
                _, device = moved((x, y, z))
                leaf = device * leaf_dev + halved(1 - e, 1)
                slot_of[i, leaf_dev * leaf_dev + x - 1] = find(halved(1 + e, 1), leaf)

    early = line * 2 < lines
    pl.when(early)(search)

    pl.semaphore_wait(barrier, expected)

    def line_copy(j, ref, rows, which):
        block = ref.at[pl.ds(pl.multiple_of(line * rows, rows), rows), :]
        return pltpu.make_async_remote_copy(
            src_ref=block,
            dst_ref=block,
            send_sem=group_send.at[which],
            recv_sem=group_recv.at[which],
            device_id=(lax.rem(line + j, lines) * plane + spot,),
            device_id_type=MESH,
        )

    def plane_copy(r, source, target, which):
        return pltpu.make_async_remote_copy(
            src_ref=source,
            dst_ref=target,
            send_sem=group_send.at[which],
            recv_sem=group_recv.at[which],
            device_id=(peer(r),),
            device_id_type=MESH,
        )

    def everything(which):
        whole = {
            COEFS: coefs.at[pl.ds(0, (lines - 1) * own_rows), :],
            TERMS: terms.at[pl.ds(1, plane - 1)],
            CLUSTERS: clusters.at[pl.ds(0, (lines - 1) * teams * half), :],
            SUMS: sums,
        }[which]
        return plane_copy(1, whole, whole, which)

    def panel_copy(kind, e, source, receiver):
        first, count = (0, leaf_dev) if kind[0] == 0 else (halved(1 - e, 1), 1)
        rows = panels.at[pl.ds(source * leaf_dev + first, count)]
        at = (kind[0] * kinds[1] + kind[1]) * kinds[2] + kind[2]
        return pltpu.make_async_remote_copy(
            src_ref=rows,
            dst_ref=rows,
            send_sem=panel_send.at[at],
            recv_sem=panel_recv.at[at],
            device_id=(receiver,),
            device_id_type=MESH,
        )

    def sends(kind, act):
        a = 1 if kind[1] else 0 if kind[0] else 2
        hop = tuple(k if b == a else 0 for b, k in enumerate(kind))
        rest = tuple(0 if b == a else k for b, k in enumerate(kind))
        ok, to = moved(hop)
        known, source = moved(rest)
        e = offset(0, kind[0]) * (-1 if a == 0 else 1)
        when(kind, ok & known, lambda: act(panel_copy(kind, e, source, to)))

    def receives(kind):
        known, source = moved(kind)
        copy = panel_copy(kind, offset(0, kind[0]), source, peer(1))
        when(kind, known, lambda: copy.wait_recv())

    def start(copy):
        copy.start()

    @pl.loop(1, lines)
    def _(j):
        line_copy(lines - j, coefs, own_rows, COEFS).start()

    for z in reversed(along_z):
        sends((0, 0, z), start)
    for x in along_x:
        sends((x, 0, 0), start)
    for y in reversed(along_y):
        sends((0, y, 0), start)

    term = None
    for l in range(leaf_dev):
        part = lax.dot_general(transfer[l], flats[l], TN, preferred_element_type=F32)
        term = part if term is None else term + part
    terms[0] = packed(term, leaf_dev * rank)

    for r in reversed(range(1, plane)):
        plane_copy(r, terms.at[0], terms.at[r], TERMS).start()

    loads[4].wait()
    loads[5].start()

    chunk = min(8 // leaf_dev, lines)
    chunks = lines // chunk
    mine = lax.div(me, group)
    parent = coords_of(mine, axis_bits(0, bit_count - 3))
    parents = bit_count - 3
    candidates = min(2 ** (parents - 3), 27)

    @pl.loop(0, candidates)
    def _(i):
        upper, _, ok = candidate(parent, parents, i)
        for h in range(8):
            d = [2 * upper[a] + (h >> a & 1) - parent[a] for a in range(3)]
            use = ok & ((jnp.abs(d[0]) > 1) | (jnp.abs(d[1]) > 1) | (jnp.abs(d[2]) > 1))
            code = jnp.where(use, code_of(d), shifts)
            mats1[i, h * half : (h + 1) * half, :] = extract(coupling, code, 1, spread, h * rank)

    here = coords_of(line * plane, bits)
    base = coords_of(spot, bits)

    def leaf_mats(c):
        for r in range(plane):
            goal = list(base)
            for a in range(3):
                for p, b in enumerate(bits[a]):
                    if b < plane_bits and r >> b & 1:
                        goal[a] = goal[a] + (1 - 2 * bit_of(spot, b)) * 2**p
            target = [here[a] + goal[a] for a in range(3)]
            for j in range(chunk):
                there = coords_of((c * chunk + j) * plane, bits)
                source = [there[a] + base[a] for a in range(3)]
                d = [source[a] - target[a] for a in range(3)]
                close = jnp.abs(d[0]) <= 1
                for a in (1, 2):
                    close = close & (jnp.abs(halved(source[a], 1) - halved(target[a], 1)) <= 1)
                apart = (jnp.abs(d[1]) > 1) | (jnp.abs(d[2]) > 1)
                parts = {}
                for e in range(1 - leaf_dev, leaf_dev):
                    dx = leaf_dev * d[0] + e
                    use = close & (apart | (jnp.abs(dx) > 1))
                    code = jnp.where(use, code_of([dx, d[1], d[2]]), shifts)
                    at = ((r % 2 * chunk + j) * (2 * leaf_dev - 1) + e + leaf_dev - 1) * rank
                    parts[e] = extract(coupling, code, 0, spread, at)
                for m in range(leaf_dev):
                    rows = slice((j * leaf_dev + m) * half, (j * leaf_dev + m + 1) * half)
                    for l in range(leaf_dev):
                        mats0[c * plane + r, rows, 2 * rank * l : 2 * rank * (l + 1)] = parts[m - l]

    if chunks == 1:
        leaf_mats(0)
    else:
        pl.loop(0, chunks)(leaf_mats)

    for x in along_x:
        receives((x, 0, 0))
        for y in reversed(along_y):
            sends((x, y, 0), start)
    receives((0, 0, 1))
    for x in along_x:
        sends((x, 0, 1), start)
    for y in reversed(along_y):
        sends((0, y, 1), start)

    pl.when(~early)(search)

    everything(TERMS).wait_recv()
    for t in range(teams):
        total = None
        for r in range(t * group, (t + 1) * group):
            part = terms[r].astype(F32)
            total = part if total is None else total + part
        at = (line * teams + flipped(lax.div(spot, group), t, teams.bit_length() - 1)) * half
        clusters[pl.ds(pl.multiple_of(at, half), half), :] = total.astype(BF16)

    @pl.loop(1, lines)
    def _(j):
        line_copy(lines - j, clusters, teams * half, CLUSTERS).start()

    for z in along_z:
        if z > 1:
            receives((0, 0, z))
            for x in along_x:
                sends((x, 0, z), start)
            for y in reversed(along_y):
                sends((0, y, z), start)

    everything(COEFS).wait_recv()
    wide = lax.broadcasted_iota(jnp.int32, (cols, 2 * rank), 1) < rank
    depth = chunk * own_rows
    for r in reversed(range(plane)):
        total = None
        for c in range(chunks):
            part = lax.dot_general(
                coefs[c * depth : (c + 1) * depth, :],
                mats0[c * plane + r],
                TN,
                preferred_element_type=F32,
            )
            total = part if total is None else total + part
        one, two = total[:, : 2 * rank], total[:, 2 * rank :]
        straight = jnp.where(wide, one[:cols], two[cols:])
        crossed = jnp.where(wide, two[:cols], one[cols:])
        result = straight + pltpu.roll(crossed, rank, 1)
        if r == 0:
            kept[...] = result
        else:
            sent[r - 1] = result.astype(BF16)
    for r in reversed(range(1, plane)):
        plane_copy(r, sent.at[r - 1], sums.at[r - 1], SUMS).start()

    for z in along_z:
        for x in along_x:
            receives((x, 0, z))
            for y in reversed(along_y):
                sends((x, y, z), start)

    loads[5].wait()

    def near_part(y):
        totals = [None] * leaf_dev
        outer = [None] * len(along_x)

        def add(old, panel, l, slot):
            part = jnp.dot(panel, blocks[l, slot], preferred_element_type=F32)
            return part if old is None else old + part

        for z in range(kinds[2]):
            at = y * kinds[2] + z
            ok, device = moved((0, y, z))
            for m in range(leaf_dev):
                panel = panels[device * leaf_dev + m]
                if y > 1 or z > 1:
                    panel = jnp.where(ok, panel, jnp.zeros_like(panel))
                for l in range(leaf_dev):
                    totals[l] = add(totals[l], panel, l, slot_of[at, l * leaf_dev + m])
            for x in along_x:
                e = offset(0, x)
                ok, device = moved((x, y, z))
                panel = panels[device * leaf_dev + halved(1 - e, 1)]
                if x > 1 or y > 1 or z > 1:
                    panel = jnp.where(ok, panel, jnp.zeros_like(panel))
                slot = slot_of[at, leaf_dev * leaf_dev + x - 1]
                outer[x - 1] = add(outer[x - 1], panel, halved(1 + e, 1), slot)
        for l in range(leaf_dev):
            near[l] = totals[l] if y == 0 else near[l] + totals[l]
        for x in along_x:
            l = halved(1 + offset(0, x), 1)
            near[l] = near[l] + outer[x - 1]

    near_part(0)

    if lines > 1:
        everything(CLUSTERS).wait_recv()

    def step(i, total):
        _, q, _ = candidate(parent, parents, i)
        rows = pl.ds(pl.multiple_of(q * 8 * half, 8 * half), 8 * half)
        return total + lax.dot_general(clusters[rows, :], mats1[i], TN, preferred_element_type=F32)

    total = lax.fori_loop(0, candidates, step, jnp.zeros((2 * cols, 2 * rank), F32))
    down = (total[:cols, :rank] + total[cols:, rank:]).astype(BF16)
    lower = [
        lax.dot_general(down, transfer[l], NT, preferred_element_type=F32) for l in range(leaf_dev)
    ]
    kept[...] = kept[...] + jnp.concatenate(lower, axis=1)

    for y in along_y:
        for x in range(kinds[0]):
            for z in range(kinds[2]):
                receives((x, y, z))
        near_part(y)

    every = [
        (x, y, z)
        for x in range(kinds[0])
        for y in range(kinds[1])
        for z in range(kinds[2])
        if x or y or z
    ]
    for kind in every:
        sends(kind, lambda copy: copy.wait_send())
    everything(COEFS).wait_send()
    everything(TERMS).wait_send()
    everything(CLUSTERS).wait_send()

    everything(SUMS).wait_recv()
    total = kept[...]
    for r in range(plane - 1):
        total = total + sums[r].astype(F32)
    total = total.astype(BF16).astype(F32)
    pair = jnp.concatenate([jnp.where(wide, total, 0.0), jnp.where(wide, 0.0, total)], axis=0)
    far = jnp.dot(
        pair.astype(BF16),
        basis[...].reshape(leaf_dev * rank, points),
        preferred_element_type=F32,
    )
    for l in range(leaf_dev):
        out[l] = (near[l] + far[l * cols : (l + 1) * cols]).astype(BF16)
    everything(SUMS).wait_send()


def per_device(panels, basis, transfer, near_blocks, coupling, near_list):
    n = lax.axis_size("leaf")
    leaf_dev, cols, points = panels.shape
    rank = basis.shape[1]
    slots = near_list.shape[1]
    shifts = coupling.shape[1]
    half = rank // 2
    leaves = n * leaf_dev
    coupling = coupling.transpose(1, 0, 2).reshape(shifts, 2, half, 2 * rank)
    coupling = coupling.transpose(0, 2, 1, 3).reshape(shifts, rank, 2 * rank)
    plane = min(8, n)
    lines = n // plane
    teams = plane * leaf_dev // 8
    chunk = min(8 // leaf_dev, lines)
    kinds = [min(2 ** len(b), 3) for b in axis_bits(leaf_dev.bit_length() - 1, n.bit_length() - 1)]
    faces = kinds[0] * kinds[1] * kinds[2]
    dma = pltpu.SemaphoreType.DMA
    return pl.pallas_call(
        functools.partial(kernel, n),
        out_shape=pltpu.VMEM(panels.shape, BF16),
        in_specs=[pl.BlockSpec(memory_space=pl.ANY)] * 6,
        out_specs=pl.BlockSpec(memory_space=pltpu.VMEM),
        scratch_shapes=[
            pltpu.VMEM((leaves, cols, points), BF16),
            pltpu.VMEM(basis.shape, BF16),
            pltpu.VMEM(transfer.shape, BF16),
            pltpu.VMEM(near_blocks.shape, BF16),
            pltpu.VMEM((shifts + 1, rank, 2 * rank), BF16),
            pltpu.SMEM(near_list.shape, jnp.int32),
            pltpu.SMEM((kinds[1] * kinds[2], leaf_dev * leaf_dev + 2), jnp.int32),
            pltpu.VMEM((max(2 * chunk * (2 * leaf_dev - 1), 8) * rank, 2 * rank), F32),
            pltpu.VMEM(
                (plane * (lines // chunk), chunk * leaf_dev * half, 2 * rank * leaf_dev), BF16
            ),
            pltpu.VMEM((min(leaves // 64, 27), 8 * half, 2 * rank), BF16),
            pltpu.VMEM((lines * leaf_dev * half, 2 * cols), BF16),
            pltpu.VMEM((plane, half, 2 * cols), BF16),
            pltpu.VMEM((lines * teams * half, 2 * cols), BF16),
            pltpu.VMEM((cols, leaf_dev * rank), F32),
            pltpu.VMEM((plane - 1, cols, leaf_dev * rank), BF16),
            pltpu.VMEM((plane - 1, cols, leaf_dev * rank), BF16),
            pltpu.VMEM((leaf_dev, cols, points), F32),
            dma((6,)),
            dma((faces,)),
            dma((faces,)),
            dma((4,)),
            dma((4,)),
        ],
        compiler_params=pltpu.CompilerParams(
            collective_id=0, has_side_effects=True, vmem_limit_bytes=60 * 2**20
        ),
    )(panels, basis, transfer, near_blocks, coupling, near_list)


def solution(mesh):
    placed = (
        P("leaf", None, None),
        P("leaf", None, None),
        P("leaf", None, None),
        P("leaf", None, None, None),
        P(),
        P("leaf", None),
    )
    return jax.shard_map(
        per_device, mesh=mesh, in_specs=placed, out_specs=P("leaf", None, None), check_vma=False
    )
```

```python
import functools

import jax
import jax.numpy as jnp
from jax import lax
from jax.experimental import pallas as pl
from jax.experimental.pallas import tpu as pltpu
from jax.sharding import PartitionSpec as P

MESH = pl.DeviceIdType.MESH
F32 = jnp.float32
BF16 = jnp.bfloat16
REACH = 3
SPAN = 2 * REACH + 1
TN = (((0,), (0,)), ((), ()))
NT = (((1,), (1,)), ((), ()))
COEFS, SUMS = range(2)


def axis_bits(first, bit_count):
    return [[b for b in range(bit_count) if (b + first) % 3 == a] for a in range(3)]


def halved(index, times):
    return index // 2**times if isinstance(index, int) else lax.div(index, 2**times)


def bit_of(index, b):
    high = halved(index, b) if b else index
    return high % 2 if isinstance(index, int) else lax.rem(high, 2)


def coords_of(index, bits):
    return [
        sum(bit_of(index, b) * 2**p for p, b in enumerate(bits[a])) + index * 0 for a in range(3)
    ]


def index_of(coords, bits):
    return sum(bit_of(coords[a], p) * 2**b for a in range(3) for p, b in enumerate(bits[a]))


def inside(coords, bits):
    ok = None
    for a in range(3):
        here = (coords[a] >= 0) & (coords[a] < 2 ** len(bits[a]))
        ok = here if ok is None else ok & here
    return ok


def flipped(index, mask, bit_count):
    result = 0
    for b in range(bit_count):
        one, two = bit_of(index, b), bit_of(mask, b)
        result = result + (one + two - 2 * one * two) * 2**b
    return result


def extract(coupling, code, level, spread, at):
    half = coupling.shape[1] // 2
    spread[at : at + 2 * half, :] = coupling[code].astype(F32)
    return spread[pl.ds(at + level, half, stride=2), :].astype(BF16)


def code_of(d):
    return (SPAN * (d[0] + REACH) + d[1] + REACH) * SPAN + d[2] + REACH


def kernel(
    n,
    panels_hbm,
    basis_hbm,
    transfer_hbm,
    blocks_hbm,
    coupling_hbm,
    near_hbm,
    out,
    panels,
    basis,
    transfer,
    blocks,
    coupling,
    near_list,
    slot_of,
    spread,
    mats0,
    mats1,
    coefs,
    reach,
    kept,
    sent,
    sums,
    near,
    load_sem,
    panel_send,
    panel_recv,
    group_send,
    group_recv,
):
    leaf_dev, rank, points = basis.shape
    cols = panels.shape[1]
    slots = near_list.shape[1]
    shifts = coupling_hbm.shape[0]
    half = rank // 2
    low_bits = leaf_dev.bit_length() - 1
    dev_bits = n.bit_length() - 1
    bit_count = low_bits + dev_bits
    group = 8 // leaf_dev
    plane = min(8, n)
    plane_bits = plane.bit_length() - 1
    lines = n // plane
    teams = plane // group
    own_rows = (leaf_dev + 1) * half
    me = lax.axis_index("leaf")
    line, spot = lax.div(me, plane), lax.rem(me, plane)

    loads = [
        pltpu.make_async_copy(source, target, load_sem.at[i])
        for i, (source, target) in enumerate(
            [
                (panels_hbm, panels.at[pl.ds(me * leaf_dev, leaf_dev)]),
                (basis_hbm, basis),
                (transfer_hbm, transfer),
                (near_hbm, near_list),
                (coupling_hbm, coupling.at[pl.ds(0, shifts)]),
                (blocks_hbm, blocks),
            ]
        )
    ]
    for load in loads[:5]:
        load.start()

    bits = axis_bits(low_bits, dev_bits)
    where = coords_of(me, bits)
    side = [1 - 2 * bit_of(c, 0) for c in where]
    kinds = [min(2 ** len(b), 3) for b in bits]

    def offset(a, kind):
        return side[a] * bit_of(kind, 0) - side[a] * halved(kind, 1)

    def moved(kind):
        there = [where[a] + offset(a, kind[a]) for a in range(3)]
        ok = inside(there, bits)
        return ok, jnp.where(ok, index_of([jnp.maximum(v, 0) for v in there], bits), me)

    def when(kind, ok, act):
        if all(k < 2 for k in kind):
            act()
        else:
            pl.when(ok)(act)

    def peer(r):
        return line * plane + flipped(spot, r, plane_bits)

    barrier = pltpu.get_barrier_semaphore()

    def greet(device):
        pl.semaphore_signal(barrier, inc=1, device_id=(device,), device_id_type=MESH)

    @pl.loop(1, lines)
    def _(j):
        greet(lax.rem(line + j, lines) * plane + spot)

    for r in range(1, plane):
        greet(peer(r))
    faces = [tuple(k if b == a else 0 for b in range(3)) for a in range(3) for k in range(1, kinds[a])]
    expected = lines - 1 + plane - 1
    for face in faces:
        ok, to = moved(face)
        when(face, ok, lambda: greet(to))
        expected = expected + jnp.where(ok, 1, 0)

    coupling[shifts] = jnp.zeros((rank, 2 * rank), BF16)

    for load in loads[:3]:
        load.wait()
    lane = lax.broadcasted_iota(jnp.int32, (half, 2 * cols), 1)

    def packed(value, at):
        spread[at : at + rank, :] = value
        even = spread[pl.ds(at, half, stride=2), :]
        odd = spread[pl.ds(at + 1, half, stride=2), :]
        return jnp.where(lane < cols, even, odd).astype(BF16)

    def own_part(l):
        return pl.ds(pl.multiple_of((line * (leaf_dev + 1) + l) * half, half), half)

    flats = []
    for l in range(leaf_dev):
        panel = panels[me * leaf_dev + l]
        flat = lax.dot_general(
            basis[l], jnp.concatenate([panel, panel], axis=0), NT, preferred_element_type=F32
        )
        coefs[own_part(l), :] = packed(flat, l * rank)
        flats.append(flat.astype(BF16))
    term = None
    for l in range(leaf_dev):
        part = lax.dot_general(transfer[l], flats[l], TN, preferred_element_type=F32)
        term = part if term is None else term + part
    coefs[own_part(leaf_dev), :] = packed(term, leaf_dev * rank)

    along_x, along_y, along_z = (range(1, k) for k in kinds)

    def search():
        loads[3].wait()

        @pl.loop(0, kinds[1] * kinds[2])
        def _(i):
            y, z = lax.div(i, kinds[2]), lax.rem(i, kinds[2])

            def find(l, leaf):
                total = 0
                for k in range(slots):
                    total = jnp.where(near_list[l, k] == leaf, k, total)
                return total

            _, device = moved((0, y, z))
            for l in range(leaf_dev):
                for m in range(leaf_dev):
                    slot_of[i, l * leaf_dev + m] = find(l, device * leaf_dev + m)
            for x in along_x:
                e = offset(0, x)
                _, device = moved((x, y, z))
                leaf = device * leaf_dev + halved(1 - e, 1)
                slot_of[i, leaf_dev * leaf_dev + x - 1] = find(halved(1 + e, 1), leaf)

    early = line * 2 < lines
    pl.when(early)(search)

    pl.semaphore_wait(barrier, expected)

    def line_copy(j):
        block = coefs.at[pl.ds(pl.multiple_of(line * own_rows, own_rows), own_rows), :]
        return pltpu.make_async_remote_copy(
            src_ref=block,
            dst_ref=block,
            send_sem=group_send.at[COEFS],
            recv_sem=group_recv.at[COEFS],
            device_id=(lax.rem(line + j, lines) * plane + spot,),
            device_id_type=MESH,
        )

    def plane_copy(r, source, target, which):
        return pltpu.make_async_remote_copy(
            src_ref=source,
            dst_ref=target,
            send_sem=group_send.at[which],
            recv_sem=group_recv.at[which],
            device_id=(peer(r),),
            device_id_type=MESH,
        )

    def everything(which):
        whole = {
            COEFS: coefs.at[pl.ds(0, (lines - 1) * own_rows), :],
            SUMS: sums,
        }[which]
        return plane_copy(1, whole, whole, which)

    front = halved(1 + side[0], 1)

    def panel_copy(kind, lane, source, receiver):
        first, count, late = 0, leaf_dev, 0
        if kind[0]:
            first, count = lane, 1
        elif lane is not None:
            first, count, late = (front, 1 - front)[lane], 1, lane
        rows = panels.at[pl.ds(source * leaf_dev + first, count)]
        at = (kind[0] * kinds[1] + kind[1]) * kinds[2] + kind[2]
        if late:
            at = kinds[0] * kinds[1] * kinds[2] + kind[1]
        return pltpu.make_async_remote_copy(
            src_ref=rows,
            dst_ref=rows,
            send_sem=panel_send.at[at],
            recv_sem=panel_recv.at[at],
            device_id=(receiver,),
            device_id_type=MESH,
        )

    def lanes_of(kind):
        return (0, 1) if kind[0] == 0 and kind[2] > 1 else (None,)

    def hops_of(kind):
        if kind[0] and kind[1] > 1 and kind[2] > 1:
            return (kind[0], kind[1], 0)
        a = 1 if kind[1] else 0 if kind[0] else 2
        return tuple(k if b == a else 0 for b, k in enumerate(kind))

    def sends(kind, act, lane=None):
        hop = hops_of(kind)
        rest = tuple(k - h for k, h in zip(kind, hop))
        ok, to = moved(hop)
        known, source = moved(rest)
        if kind[0]:
            lane = halved(1 + offset(0, kind[0]) * (1 if hop[0] else -1), 1)
        when(kind, ok & known, lambda: act(panel_copy(kind, lane, source, to)))

    def receives(kind, lane=None):
        known, source = moved(kind)
        if kind[0]:
            lane = halved(1 - offset(0, kind[0]), 1)
        copy = panel_copy(kind, lane, source, peer(1))
        when(kind, known, lambda: copy.wait_recv())

    def start(copy):
        copy.start()

    @pl.loop(1, lines)
    def _(j):
        line_copy(lines - j).start()

    for lane in (0, 1):
        for z in along_z:
            if z > 1:
                sends((0, 0, z), start, lane)
    sends((0, 0, 1), start)
    for x in along_x:
        sends((x, 0, 0), start)
    for y in reversed(along_y):
        sends((0, y, 0), start)

    loads[4].wait()
    loads[5].start()

    chunk = min(8 // leaf_dev, lines)
    chunks = lines // chunk
    parents = bit_count - 3
    parent_bits = axis_bits(0, parents)
    team = lax.div(spot, group)

    def parent_mats(c):
        for t in range(teams):
            goal = line * teams + flipped(team, t, teams.bit_length() - 1)
            target = coords_of(goal, parent_bits)
            for j in range(chunk):
                source = coords_of((c * chunk + j) * teams + team, parent_bits)
                d = [source[a] - target[a] for a in range(3)]
                use = (jnp.abs(d[0]) > 1) | (jnp.abs(d[1]) > 1) | (jnp.abs(d[2]) > 1)
                for a in range(3):
                    use = use & (jnp.abs(halved(source[a], 1) - halved(target[a], 1)) <= 1)
                code = jnp.where(use, code_of(d), shifts)
                mat = extract(coupling, code, 1, spread, (t * chunk + j) * rank)
                rows = slice(j * half, (j + 1) * half)
                mats1[c, rows, 2 * rank * t : 2 * rank * (t + 1)] = mat

    here = coords_of(line * plane, bits)
    base = coords_of(spot, bits)

    def leaf_mats(c):
        for r in range(plane):
            goal = list(base)
            for a in range(3):
                for p, b in enumerate(bits[a]):
                    if b < plane_bits and r >> b & 1:
                        goal[a] = goal[a] + (1 - 2 * bit_of(spot, b)) * 2**p
            target = [here[a] + goal[a] for a in range(3)]
            for j in range(chunk):
                there = coords_of((c * chunk + j) * plane, bits)
                source = [there[a] + base[a] for a in range(3)]
                d = [source[a] - target[a] for a in range(3)]
                close = jnp.abs(d[0]) <= 1
                for a in (1, 2):
                    close = close & (jnp.abs(halved(source[a], 1) - halved(target[a], 1)) <= 1)
                apart = (jnp.abs(d[1]) > 1) | (jnp.abs(d[2]) > 1)
                parts = {}
                for e in range(1 - leaf_dev, leaf_dev):
                    dx = leaf_dev * d[0] + e
                    use = close & (apart | (jnp.abs(dx) > 1))
                    code = jnp.where(use, code_of([dx, d[1], d[2]]), shifts)
                    at = ((r % 2 * chunk + j) * (2 * leaf_dev - 1) + e + leaf_dev - 1) * rank
                    parts[e] = extract(coupling, code, 0, spread, at)
                for m in range(leaf_dev):
                    rows = slice((j * leaf_dev + m) * half, (j * leaf_dev + m + 1) * half)
                    for l in range(leaf_dev):
                        mats0[c * plane + r, rows, 2 * rank * l : 2 * rank * (l + 1)] = parts[m - l]

    for build in (parent_mats, leaf_mats):
        if chunks == 1:
            build(0)
        else:
            pl.loop(0, chunks)(build)

    reach[: leaf_dev * rank] = basis[...].reshape(leaf_dev * rank, points)
    for l in range(leaf_dev):
        lift = lax.dot_general(transfer[l], basis[l], TN, preferred_element_type=F32).astype(BF16)
        for p in range(2):
            at = (leaf_dev + 2 * l + p) * rank
            reach[at : at + rank] = lift

    for x in along_x:
        receives((x, 0, 0))
        for y in reversed(along_y):
            sends((x, y, 0), start)
    receives((0, 0, 1))
    for x in along_x:
        sends((x, 0, 1), start)
    for y in reversed(along_y):
        sends((0, y, 1), start)

    pl.when(~early)(search)

    everything(COEFS).wait_recv()
    wide = lax.broadcasted_iota(jnp.int32, (cols, 2 * rank), 1) < rank
    def gathered(c, first, count):
        parts = []
        for j in range(chunk):
            at = (c * chunk + j) * own_rows + first * half
            parts.append(coefs[at : at + count * half, :])
        return jnp.concatenate(parts, axis=0)

    def applied(first, count, mats, at):
        total = None
        for c in range(chunks):
            part = lax.dot_general(
                gathered(c, first, count), mats[c * at[1] + at[0]], TN, preferred_element_type=F32
            )
            total = part if total is None else total + part
        return total

    low = lax.broadcasted_iota(jnp.int32, (half, 2 * rank), 1) < rank
    every_down = applied(leaf_dev, 1, mats1, (0, 1))
    for r in reversed(range(plane)):
        total = applied(0, leaf_dev, mats0, (r, plane))
        one, two = total[:, : 2 * rank], total[:, 2 * rank :]
        straight = jnp.where(wide, one[:cols], two[cols:])
        crossed = jnp.where(wide, two[:cols], one[cols:])
        result = straight + pltpu.roll(crossed, rank, 1)
        t = r // group
        if r % group == group - 1:
            one = every_down[:, 2 * rank * t : 2 * rank * (t + 1)]
            straight = jnp.where(low, one[:half], one[cols + half :])
            crossed = jnp.where(low, one[half:cols], one[cols : cols + half])
            down = straight + pltpu.roll(crossed, rank, 1)
        if r == 0:
            kept[:cols] = result
            kept[cols:] = down
        else:
            sent[r - 1, :cols] = result.astype(BF16)
            sent[r - 1, cols:] = down.astype(BF16)
    for r in reversed(range(1, plane)):
        plane_copy(r, sent.at[r - 1], sums.at[r - 1], SUMS).start()

    if kinds[2] > 2:
        for lane in (0, 1):
            receives((0, 0, 2), lane)
            x = 1 + lane
            if x in along_x:
                sends((x, 0, 2), start)
                if kinds[1] > 2:
                    sends((x, 2, 2), start)
            for y in reversed(along_y):
                sends((0, y, 2), start, lane)

    for x in along_x:
        receives((x, 0, 1))
        for y in reversed(along_y):
            sends((x, y, 1), start)

    def near_part(y, levels, first=False):
        totals = [None] * leaf_dev
        outer = [None] * len(along_x)

        def add(old, panel, l, slot):
            part = jnp.dot(panel, blocks[l, slot], preferred_element_type=F32)
            return part if old is None else old + part

        for z in levels:
            at = y * kinds[2] + z
            _, device = moved((0, y, z))
            for m in range(leaf_dev):
                panel = panels[device * leaf_dev + m]
                for l in range(leaf_dev):
                    totals[l] = add(totals[l], panel, l, slot_of[at, l * leaf_dev + m])
            for x in along_x:
                e = offset(0, x)
                ok, device = moved((x, y, z))
                panel = panels[device * leaf_dev + halved(1 - e, 1)]
                if x > 1:
                    panel = jnp.where(ok, panel, jnp.zeros_like(panel))
                slot = slot_of[at, leaf_dev * leaf_dev + x - 1]
                outer[x - 1] = add(outer[x - 1], panel, halved(1 + e, 1), slot)
        for l in range(leaf_dev):
            near[l] = totals[l] if first else near[l] + totals[l]
        for x in along_x:
            l = halved(1 + offset(0, x), 1)
            near[l] = near[l] + outer[x - 1]

    def near_when(y, levels):
        for x in range(kinds[0]):
            for z in levels:
                if (x, y, z) not in taken:
                    for lane in lanes_of((x, y, z)):
                        receives((x, y, z), lane)
        kind = (0, y, max(levels))
        when(kind, moved(kind)[0], lambda: near_part(y, levels))

    taken = [(x, 0, 1) for x in range(kinds[0])] + [(x, 0, 0) for x in range(kinds[0])]
    taken += [(0, 0, 2)]
    loads[5].wait()
    near_part(0, range(2), first=True)
    for y in along_y:
        near_when(y, range(2))
    if kinds[2] > 2:
        for x in along_x:
            receives((x, 0, 2))
            sends((x, 1, 2), start)
            taken.append((x, 0, 2))
        near_when(0, [2])
        near_when(1, [2])

    if kinds[1] > 2 and kinds[2] > 2:
        near_when(2, [2])

    every = [
        (x, y, z)
        for x in range(kinds[0])
        for y in range(kinds[1])
        for z in range(kinds[2])
        if x or y or z
    ]
    for kind in every:
        for lane in lanes_of(kind):
            sends(kind, lambda copy: copy.wait_send(), lane)
    everything(COEFS).wait_send()

    everything(SUMS).wait_recv()
    total = kept[...]
    for r in range(plane - 1):
        total = total + sums[r].astype(F32)
    leafs, down = total[:cols], total[cols:]
    none = jnp.zeros_like(leafs)
    down = jnp.concatenate([jnp.where(low, down, 0.0), jnp.where(low, 0.0, down)], axis=0)
    pair = jnp.concatenate(
        [
            jnp.concatenate([jnp.where(wide, leafs, 0.0), jnp.where(wide, 0.0, leafs)], axis=0),
            jnp.concatenate([down, none], axis=0),
            jnp.concatenate([none, down], axis=0),
        ],
        axis=1,
    )
    far = jnp.dot(pair.astype(BF16), reach[...], preferred_element_type=F32)
    for l in range(leaf_dev):
        out[l] = (near[l] + far[l * cols : (l + 1) * cols]).astype(BF16)
    everything(SUMS).wait_send()


def per_device(panels, basis, transfer, near_blocks, coupling, near_list):
    n = lax.axis_size("leaf")
    leaf_dev, cols, points = panels.shape
    rank = basis.shape[1]
    slots = near_list.shape[1]
    shifts = coupling.shape[1]
    half = rank // 2
    leaves = n * leaf_dev
    coupling = coupling.transpose(1, 0, 2).reshape(shifts, 2, half, 2 * rank)
    coupling = coupling.transpose(0, 2, 1, 3).reshape(shifts, rank, 2 * rank)
    plane = min(8, n)
    lines = n // plane
    teams = plane * leaf_dev // 8
    chunk = min(8 // leaf_dev, lines)
    kinds = [min(2 ** len(b), 3) for b in axis_bits(leaf_dev.bit_length() - 1, n.bit_length() - 1)]
    faces = kinds[0] * kinds[1] * kinds[2] + kinds[1]
    dma = pltpu.SemaphoreType.DMA
    return pl.pallas_call(
        functools.partial(kernel, n),
        out_shape=pltpu.VMEM(panels.shape, BF16),
        in_specs=[pl.BlockSpec(memory_space=pl.ANY)] * 6,
        out_specs=pl.BlockSpec(memory_space=pltpu.VMEM),
        scratch_shapes=[
            pltpu.VMEM((leaves, cols, points), BF16),
            pltpu.VMEM(basis.shape, BF16),
            pltpu.VMEM(transfer.shape, BF16),
            pltpu.VMEM(near_blocks.shape, BF16),
            pltpu.VMEM((shifts + 1, rank, 2 * rank), BF16),
            pltpu.SMEM(near_list.shape, jnp.int32),
            pltpu.SMEM((kinds[1] * kinds[2], leaf_dev * leaf_dev + 2), jnp.int32),
            pltpu.VMEM((max(2 * chunk * (2 * leaf_dev - 1), 8) * rank, 2 * rank), F32),
            pltpu.VMEM(
                (plane * (lines // chunk), chunk * leaf_dev * half, 2 * rank * leaf_dev), BF16
            ),
            pltpu.VMEM((lines // chunk, chunk * half, 2 * rank * teams), BF16),
            pltpu.VMEM((lines * (leaf_dev + 1) * half, 2 * cols), BF16),
            pltpu.VMEM((3 * leaf_dev * rank, points), BF16),
            pltpu.VMEM((cols + half, leaf_dev * rank), F32),
            pltpu.VMEM((plane - 1, cols + half, leaf_dev * rank), BF16),
            pltpu.VMEM((plane - 1, cols + half, leaf_dev * rank), BF16),
            pltpu.VMEM((leaf_dev, cols, points), F32),
            dma((6,)),
            dma((faces,)),
            dma((faces,)),
            dma((2,)),
            dma((2,)),
        ],
        compiler_params=pltpu.CompilerParams(
            collective_id=0, has_side_effects=True, vmem_limit_bytes=60 * 2**20
        ),
    )(panels, basis, transfer, near_blocks, coupling, near_list)


def solution(mesh):
    placed = (
        P("leaf", None, None),
        P("leaf", None, None),
        P("leaf", None, None),
        P("leaf", None, None, None),
        P(),
        P("leaf", None),
    )
    return jax.shard_map(
        per_device, mesh=mesh, in_specs=placed, out_specs=P("leaf", None, None), check_vma=False
    )
```

```python
import functools

import jax
import jax.numpy as jnp
from jax import lax
from jax.experimental import pallas as pl
from jax.experimental.pallas import tpu as pltpu
from jax.sharding import PartitionSpec as P

MESH = pl.DeviceIdType.MESH
F32 = jnp.float32
BF16 = jnp.bfloat16
REACH = 3
SPAN = 2 * REACH + 1
TN = (((0,), (0,)), ((), ()))
NT = (((1,), (1,)), ((), ()))
COEFS, PAIR, SUMS = range(3)


def axis_bits(first, bit_count):
    return [[b for b in range(bit_count) if (b + first) % 3 == a] for a in range(3)]


def halved(index, times):
    return index // 2**times if isinstance(index, int) else lax.div(index, 2**times)


def bit_of(index, b):
    high = halved(index, b) if b else index
    return high % 2 if isinstance(index, int) else lax.rem(high, 2)


def coords_of(index, bits):
    return [
        sum(bit_of(index, b) * 2**p for p, b in enumerate(bits[a])) + index * 0 for a in range(3)
    ]


def index_of(coords, bits):
    return sum(bit_of(coords[a], p) * 2**b for a in range(3) for p, b in enumerate(bits[a]))


def inside(coords, bits):
    ok = None
    for a in range(3):
        here = (coords[a] >= 0) & (coords[a] < 2 ** len(bits[a]))
        ok = here if ok is None else ok & here
    return ok


def flipped(index, mask, bit_count):
    result = 0
    for b in range(bit_count):
        one, two = bit_of(index, b), bit_of(mask, b)
        result = result + (one + two - 2 * one * two) * 2**b
    return result


def extract(coupling, code, level, spread, at):
    half = coupling.shape[1] // 2
    spread[at : at + 2 * half, :] = coupling[code].astype(F32)
    return spread[pl.ds(at + level, half, stride=2), :].astype(BF16)


def code_of(d):
    return (SPAN * (d[0] + REACH) + d[1] + REACH) * SPAN + d[2] + REACH


def kernel(
    n,
    panels_hbm,
    basis_hbm,
    transfer_hbm,
    blocks_hbm,
    coupling_hbm,
    near_hbm,
    out,
    panels,
    basis,
    transfer,
    blocks,
    coupling,
    near_list,
    slot_of,
    spread,
    mats0,
    mats1,
    coefs,
    reach,
    kept,
    pair_sent,
    pair_in,
    sent,
    sums,
    near,
    load_sem,
    panel_send,
    panel_recv,
    group_send,
    group_recv,
):
    leaf_dev, rank, points = basis.shape
    cols = panels.shape[1]
    slots = near_list.shape[1]
    shifts = coupling_hbm.shape[0]
    half = rank // 2
    low_bits = leaf_dev.bit_length() - 1
    dev_bits = n.bit_length() - 1
    bit_count = low_bits + dev_bits
    group = 8 // leaf_dev
    plane = min(8, n)
    plane_bits = plane.bit_length() - 1
    lines = n // plane
    teams = plane // group
    own_rows = (leaf_dev + 1) * half
    me = lax.axis_index("leaf")
    line, spot = lax.div(me, plane), lax.rem(me, plane)

    loads = [
        pltpu.make_async_copy(source, target, load_sem.at[i])
        for i, (source, target) in enumerate(
            [
                (panels_hbm, panels.at[pl.ds(me * leaf_dev, leaf_dev)]),
                (basis_hbm, basis),
                (transfer_hbm, transfer),
                (near_hbm, near_list),
                (coupling_hbm, coupling.at[pl.ds(0, shifts)]),
                (blocks_hbm, blocks),
            ]
        )
    ]
    for load in loads[:5]:
        load.start()

    bits = axis_bits(low_bits, dev_bits)
    where = coords_of(me, bits)
    side = [1 - 2 * bit_of(c, 0) for c in where]
    kinds = [min(2 ** len(b), 3) for b in bits]

    def offset(a, kind):
        return side[a] * bit_of(kind, 0) - side[a] * halved(kind, 1)

    def moved(kind):
        there = [where[a] + offset(a, kind[a]) for a in range(3)]
        ok = inside(there, bits)
        return ok, jnp.where(ok, index_of([jnp.maximum(v, 0) for v in there], bits), me)

    def when(kind, ok, act):
        if all(k < 2 for k in kind):
            act()
        else:
            pl.when(ok)(act)

    def peer(r):
        return line * plane + flipped(spot, r, plane_bits)

    barrier = pltpu.get_barrier_semaphore()

    def greet(device):
        pl.semaphore_signal(barrier, inc=1, device_id=(device,), device_id_type=MESH)

    @pl.loop(1, lines)
    def _(j):
        greet(lax.rem(line + j, lines) * plane + spot)

    for r in range(1, plane):
        greet(peer(r))
    faces = [tuple(k if b == a else 0 for b in range(3)) for a in range(3) for k in range(1, kinds[a])]
    expected = lines - 1 + plane - 1
    for face in faces:
        ok, to = moved(face)
        when(face, ok, lambda: greet(to))
        expected = expected + jnp.where(ok, 1, 0)

    coupling[shifts] = jnp.zeros((rank, 2 * rank), BF16)

    for load in loads[:3]:
        load.wait()
    lane = lax.broadcasted_iota(jnp.int32, (half, 2 * cols), 1)

    def packed(value, at):
        spread[at : at + rank, :] = value
        even = spread[pl.ds(at, half, stride=2), :]
        odd = spread[pl.ds(at + 1, half, stride=2), :]
        return jnp.where(lane < cols, even, odd).astype(BF16)

    def own_part(l):
        return pl.ds(pl.multiple_of((line * (leaf_dev + 1) + l) * half, half), half)

    flats = []
    for l in range(leaf_dev):
        panel = panels[me * leaf_dev + l]
        flat = lax.dot_general(
            basis[l], jnp.concatenate([panel, panel], axis=0), NT, preferred_element_type=F32
        )
        coefs[own_part(l), :] = packed(flat, l * rank)
        flats.append(flat.astype(BF16))
    term = None
    for l in range(leaf_dev):
        part = lax.dot_general(transfer[l], flats[l], TN, preferred_element_type=F32)
        term = part if term is None else term + part
    coefs[own_part(leaf_dev), :] = packed(term, leaf_dev * rank)

    along_x, along_y, along_z = (range(1, k) for k in kinds)

    def search():
        loads[3].wait()

        @pl.loop(0, kinds[1] * kinds[2])
        def _(i):
            y, z = lax.div(i, kinds[2]), lax.rem(i, kinds[2])

            def find(l, leaf):
                total = 0
                for k in range(slots):
                    total = jnp.where(near_list[l, k] == leaf, k, total)
                return total

            _, device = moved((0, y, z))
            for l in range(leaf_dev):
                for m in range(leaf_dev):
                    slot_of[i, l * leaf_dev + m] = find(l, device * leaf_dev + m)
            for x in along_x:
                e = offset(0, x)
                _, device = moved((x, y, z))
                leaf = device * leaf_dev + halved(1 - e, 1)
                slot_of[i, leaf_dev * leaf_dev + x - 1] = find(halved(1 + e, 1), leaf)

    early = line * 2 < lines
    pl.when(early)(search)

    pl.semaphore_wait(barrier, expected)

    def line_copy(j):
        block = coefs.at[pl.ds(pl.multiple_of(line * own_rows, own_rows), own_rows), :]
        return pltpu.make_async_remote_copy(
            src_ref=block,
            dst_ref=block,
            send_sem=group_send.at[COEFS],
            recv_sem=group_recv.at[COEFS],
            device_id=(j * plane + spot,),
            device_id_type=MESH,
        )

    def plane_copy(r, source, target, which):
        return pltpu.make_async_remote_copy(
            src_ref=source,
            dst_ref=target,
            send_sem=group_send.at[which],
            recv_sem=group_recv.at[which],
            device_id=(peer(r),),
            device_id_type=MESH,
        )

    def everything(which):
        whole = {
            COEFS: coefs.at[pl.ds(0, (lines - 1) * own_rows), :],
            PAIR: pair_in,
            SUMS: sums,
        }[which]
        return plane_copy(1, whole, whole, which)

    front = halved(1 + side[0], 1)

    def semaphores(kind, late=0):
        far = [int(k > 1) for k in kind]
        if far[0]:
            at = kind[1] * kinds[2] + kind[2]
            return 4 + at, 10 + at
        if kind[1]:
            at = 4 + kind[1] + 2 * far[2]
        elif kind[0]:
            at = (1, 2, 9)[kind[2]]
        else:
            at = (0, 0, 3 + late)[kind[2]]
        return 2 * far[1] + far[2], at

    def panel_copy(kind, lane, source, receiver):
        first, count, late = 0, leaf_dev, 0
        if kind[0]:
            first, count = lane, 1
        elif lane is not None:
            first, count, late = (front, 1 - front)[lane], 1, lane
        rows = panels.at[pl.ds(source * leaf_dev + first, count)]
        from_at, to_at = semaphores(kind, late)
        return pltpu.make_async_remote_copy(
            src_ref=rows,
            dst_ref=rows,
            send_sem=panel_send.at[from_at],
            recv_sem=panel_recv.at[to_at],
            device_id=(receiver,),
            device_id_type=MESH,
        )

    def lanes_of(kind):
        return (0, 1) if kind[0] == 0 and kind[2] > 1 else (None,)

    def hops_of(kind):
        if kind[0] and kind[1] > 1 and kind[2]:
            return (kind[0], kind[1], 0)
        a = 1 if kind[1] else 0 if kind[0] else 2
        return tuple(k if b == a else 0 for b, k in enumerate(kind))

    def sends(kind, act, lane=None):
        hop = hops_of(kind)
        rest = tuple(k - h for k, h in zip(kind, hop))
        ok, to = moved(hop)
        known, source = moved(rest)
        if kind[0]:
            lane = halved(1 + offset(0, kind[0]) * (1 if hop[0] else -1), 1)
        when(kind, ok & known, lambda: act(panel_copy(kind, lane, source, to)))

    def whole(count, from_at, to_at):
        rows = panels.at[pl.ds(0, count)]
        return pltpu.make_async_remote_copy(
            src_ref=rows,
            dst_ref=rows,
            send_sem=panel_send.at[from_at],
            recv_sem=panel_recv.at[to_at],
            device_id=(peer(1),),
            device_id_type=MESH,
        )

    def arrived(members, lane=None):
        count = 0
        for kind in members:
            if kind[0] > 1:
                single = whole(1, *semaphores(kind))
                when(kind, moved(kind)[0], lambda: single.wait_recv())
            else:
                count += leaf_dev if kind[0] == 0 and lane is None else 1
                from_at, to_at = semaphores(kind, lane or 0)
                last = kind
        if count:
            copy = whole(count, from_at, to_at)
            when(last, moved(last)[0], lambda: copy.wait_recv())

    def start(copy):
        copy.start()

    def gather(first, last):
        @pl.loop(first, last)
        def _(j):
            @pl.when(j != line)
            def _():
                line_copy(j).start()

    gather(0, max(lines // 4, 1))
    if kinds[2] > 2:
        sends((0, 0, 2), start, 0)
    gather(max(lines // 4, 1), lines)

    if kinds[2] > 2:
        sends((0, 0, 2), start, 1)
    sends((0, 0, 1), start)
    for x in along_x:
        sends((x, 0, 0), start)
    for y in reversed(along_y):
        sends((0, y, 0), start)

    loads[4].wait()
    loads[5].start()

    chunk = min(8 // leaf_dev, lines)
    chunks = lines // chunk
    parents = bit_count - 3
    parent_bits = axis_bits(0, parents)
    team = lax.div(spot, group)

    def parent_mats(c):
        for t in range(teams):
            goal = line * teams + flipped(team, t, teams.bit_length() - 1)
            target = coords_of(goal, parent_bits)
            for j in range(chunk):
                source = coords_of((c * chunk + j) * teams + team, parent_bits)
                d = [source[a] - target[a] for a in range(3)]
                use = (jnp.abs(d[0]) > 1) | (jnp.abs(d[1]) > 1) | (jnp.abs(d[2]) > 1)
                for a in range(3):
                    use = use & (jnp.abs(halved(source[a], 1) - halved(target[a], 1)) <= 1)
                code = jnp.where(use, code_of(d), shifts)
                mat = extract(coupling, code, 1, spread, (t * chunk + j) * rank)
                rows = slice(j * half, (j + 1) * half)
                mats1[c, rows, 2 * rank * t : 2 * rank * (t + 1)] = mat

    here = coords_of(line * plane, bits)
    base = coords_of(spot, bits)

    def leaf_mats(c):
        for r in range(plane):
            goal = list(base)
            for a in range(3):
                for p, b in enumerate(bits[a]):
                    if b < plane_bits and r >> b & 1:
                        goal[a] = goal[a] + (1 - 2 * bit_of(spot, b)) * 2**p
            target = [here[a] + goal[a] for a in range(3)]
            for j in range(chunk):
                there = coords_of((c * chunk + j) * plane, bits)
                source = [there[a] + base[a] for a in range(3)]
                d = [source[a] - target[a] for a in range(3)]
                close = jnp.abs(d[0]) <= 1
                for a in (1, 2):
                    close = close & (jnp.abs(halved(source[a], 1) - halved(target[a], 1)) <= 1)
                apart = (jnp.abs(d[1]) > 1) | (jnp.abs(d[2]) > 1)
                parts = {}
                for e in range(1 - leaf_dev, leaf_dev):
                    dx = leaf_dev * d[0] + e
                    use = close & (apart | (jnp.abs(dx) > 1))
                    code = jnp.where(use, code_of([dx, d[1], d[2]]), shifts)
                    at = ((r % 2 * chunk + j) * (2 * leaf_dev - 1) + e + leaf_dev - 1) * rank
                    parts[e] = extract(coupling, code, 0, spread, at)
                for m in range(leaf_dev):
                    rows = slice((j * leaf_dev + m) * half, (j * leaf_dev + m + 1) * half)
                    for l in range(leaf_dev):
                        mats0[c * plane + r, rows, 2 * rank * l : 2 * rank * (l + 1)] = parts[m - l]

    for build in (parent_mats, leaf_mats):
        if chunks == 1:
            build(0)
        else:
            pl.loop(0, chunks)(build)

    reach[: leaf_dev * rank] = basis[...].reshape(leaf_dev * rank, points)
    for l in range(leaf_dev):
        lift = lax.dot_general(transfer[l], basis[l], TN, preferred_element_type=F32).astype(BF16)
        for p in range(2):
            at = (leaf_dev + 2 * l + p) * rank
            reach[at : at + rank] = lift

    for x in along_x:
        arrived([(x, 0, 0)])
        for y in reversed(along_y):
            sends((x, y, 0), start)
    arrived([(0, 0, 1)])
    for x in along_x:
        sends((x, 0, 1), start)
        if kinds[1] > 2:
            sends((x, 2, 1), start)
    for y in reversed(along_y):
        sends((0, y, 1), start)

    pl.when(~early)(search)

    everything(COEFS).wait_recv()
    wide = lax.broadcasted_iota(jnp.int32, (cols, 2 * rank), 1) < rank
    def gathered(c, first, count):
        parts = []
        for j in range(chunk):
            at = (c * chunk + j) * own_rows + first * half
            parts.append(coefs[at : at + count * half, :])
        return jnp.concatenate(parts, axis=0)

    def applied(first, count, mats, at):
        total = None
        for c in range(chunks):
            part = lax.dot_general(
                gathered(c, first, count), mats[c * at[1] + at[0]], TN, preferred_element_type=F32
            )
            total = part if total is None else total + part
        return total

    low = lax.broadcasted_iota(jnp.int32, (half, 2 * rank), 1) < rank
    every_down = applied(leaf_dev, 1, mats1, (0, 1))
    downs = []
    for t in range(teams):
        one = every_down[:, 2 * rank * t : 2 * rank * (t + 1)]
        straight = jnp.where(low, one[:half], one[cols + half :])
        crossed = jnp.where(low, one[half:cols], one[cols : cols + half])
        downs.append(straight + pltpu.roll(crossed, rank, 1))

    def partial(r):
        total = applied(0, leaf_dev, mats0, (r, plane))
        one, two = total[:, : 2 * rank], total[:, 2 * rank :]
        straight = jnp.where(wide, one[:cols], two[cols:])
        crossed = jnp.where(wide, two[:cols], one[cols:])
        return straight + pltpu.roll(crossed, rank, 1), downs[r // group]

    for i in range(plane // 2):
        result, down = partial(2 * i + 1)
        pair_sent[i, :cols] = result.astype(BF16)
        pair_sent[i, cols:] = down.astype(BF16)
    plane_copy(1, pair_sent, pair_in, PAIR).start()
    for i in range(plane // 2):
        result, down = partial(2 * i)
        kept[i, :cols] = result
        kept[i, cols:] = down
    everything(PAIR).wait_recv()
    for i in reversed(range(1, plane // 2)):
        sent[i - 1] = (kept[i] + pair_in[i].astype(F32)).astype(BF16)
    for i in reversed(range(1, plane // 2)):
        plane_copy(2 * i, sent.at[i - 1], sums.at[i - 1], SUMS).start()

    if kinds[2] > 2:
        for lane in (0, 1):
            arrived([(0, 0, 2)], lane)
            x = 1 + lane
            if x in along_x:
                sends((x, 0, 2), start)
                if kinds[1] > 2:
                    sends((x, 2, 2), start)
            for y in reversed(along_y):
                sends((0, y, 2), start, lane)

    for x in along_x:
        arrived([(x, 0, 1)])
        sends((x, 1, 1), start)

    def near_part(y, levels, first=False):
        totals = [None] * leaf_dev
        outer = [None] * len(along_x)

        def add(old, panel, l, slot):
            part = jnp.dot(panel, blocks[l, slot], preferred_element_type=F32)
            return part if old is None else old + part

        for z in levels:
            at = y * kinds[2] + z
            _, device = moved((0, y, z))
            for m in range(leaf_dev):
                panel = panels[device * leaf_dev + m]
                for l in range(leaf_dev):
                    totals[l] = add(totals[l], panel, l, slot_of[at, l * leaf_dev + m])
            for x in along_x:
                e = offset(0, x)
                ok, device = moved((x, y, z))
                panel = panels[device * leaf_dev + halved(1 - e, 1)]
                if x > 1:
                    panel = jnp.where(ok, panel, jnp.zeros_like(panel))
                slot = slot_of[at, leaf_dev * leaf_dev + x - 1]
                outer[x - 1] = add(outer[x - 1], panel, halved(1 + e, 1), slot)
        for l in range(leaf_dev):
            near[l] = totals[l] if first else near[l] + totals[l]
        for x in along_x:
            l = halved(1 + offset(0, x), 1)
            near[l] = near[l] + outer[x - 1]

    def near_when(y, levels):
        if y:
            arrived([(x, y, z) for x in range(kinds[0]) for z in levels])
        kind = (0, y, max(levels))
        when(kind, moved(kind)[0], lambda: near_part(y, levels))

    loads[5].wait()
    near_part(0, range(2), first=True)
    for y in along_y:
        near_when(y, range(2))
    if kinds[2] > 2:
        for x in along_x:
            arrived([(x, 0, 2)])
            sends((x, 1, 2), start)
        near_when(0, [2])
        near_when(1, [2])

    if kinds[1] > 2 and kinds[2] > 2:
        near_when(2, [2])

    every = [
        (x, y, z)
        for x in range(kinds[0])
        for y in range(kinds[1])
        for z in range(kinds[2])
        if x or y or z
    ]
    for y in range(kinds[1] - 1):
        for z in range(kinds[2] - 1):
            mine = [k for k in every if k[0] < 2 and (k[1] > 1) == y and (k[2] > 1) == z]
            last = mine[-1]
            count = sum(1 if k[0] else leaf_dev for k in mine)
            copy = whole(count, *semaphores(last))
            when(last, moved((0,) + last[1:])[0], lambda: copy.wait_send())
    for kind in every:
        if kind[0] > 1:
            sends(kind, lambda copy: copy.wait_send())
    everything(COEFS).wait_send()
    everything(PAIR).wait_send()

    everything(SUMS).wait_recv()
    total = kept[0] + pair_in[0].astype(F32)
    for i in range(plane // 2 - 1):
        total = total + sums[i].astype(F32)
    leafs, down = total[:cols], total[cols:]
    none = jnp.zeros_like(leafs)
    down = jnp.concatenate([jnp.where(low, down, 0.0), jnp.where(low, 0.0, down)], axis=0)
    pair = jnp.concatenate(
        [
            jnp.concatenate([jnp.where(wide, leafs, 0.0), jnp.where(wide, 0.0, leafs)], axis=0),
            jnp.concatenate([down, none], axis=0),
            jnp.concatenate([none, down], axis=0),
        ],
        axis=1,
    )
    far = jnp.dot(pair.astype(BF16), reach[...], preferred_element_type=F32)
    for l in range(leaf_dev):
        out[l] = (near[l] + far[l * cols : (l + 1) * cols]).astype(BF16)
    everything(SUMS).wait_send()


def per_device(panels, basis, transfer, near_blocks, coupling, near_list):
    n = lax.axis_size("leaf")
    leaf_dev, cols, points = panels.shape
    rank = basis.shape[1]
    slots = near_list.shape[1]
    shifts = coupling.shape[1]
    half = rank // 2
    leaves = n * leaf_dev
    coupling = coupling.transpose(1, 0, 2).reshape(shifts, 2, half, 2 * rank)
    coupling = coupling.transpose(0, 2, 1, 3).reshape(shifts, rank, 2 * rank)
    plane = min(8, n)
    lines = n // plane
    teams = plane * leaf_dev // 8
    chunk = min(8 // leaf_dev, lines)
    kinds = [min(2 ** len(b), 3) for b in axis_bits(leaf_dev.bit_length() - 1, n.bit_length() - 1)]
    wider = kinds[1] * kinds[2] if kinds[0] > 2 else 0
    dma = pltpu.SemaphoreType.DMA
    return pl.pallas_call(
        functools.partial(kernel, n),
        out_shape=pltpu.VMEM(panels.shape, BF16),
        in_specs=[pl.BlockSpec(memory_space=pl.ANY)] * 6,
        out_specs=pl.BlockSpec(memory_space=pltpu.VMEM),
        scratch_shapes=[
            pltpu.VMEM((leaves, cols, points), BF16),
            pltpu.VMEM(basis.shape, BF16),
            pltpu.VMEM(transfer.shape, BF16),
            pltpu.VMEM(near_blocks.shape, BF16),
            pltpu.VMEM((shifts + 1, rank, 2 * rank), BF16),
            pltpu.SMEM(near_list.shape, jnp.int32),
            pltpu.SMEM((kinds[1] * kinds[2], leaf_dev * leaf_dev + 2), jnp.int32),
            pltpu.VMEM((max(2 * chunk * (2 * leaf_dev - 1), 8) * rank, 2 * rank), F32),
            pltpu.VMEM(
                (plane * (lines // chunk), chunk * leaf_dev * half, 2 * rank * leaf_dev), BF16
            ),
            pltpu.VMEM((lines // chunk, chunk * half, 2 * rank * teams), BF16),
            pltpu.VMEM((lines * (leaf_dev + 1) * half, 2 * cols), BF16),
            pltpu.VMEM((3 * leaf_dev * rank, points), BF16),
            pltpu.VMEM((plane // 2, cols + half, leaf_dev * rank), F32),
            pltpu.VMEM((plane // 2, cols + half, leaf_dev * rank), BF16),
            pltpu.VMEM((plane // 2, cols + half, leaf_dev * rank), BF16),
            pltpu.VMEM((plane // 2 - 1, cols + half, leaf_dev * rank), BF16),
            pltpu.VMEM((plane // 2 - 1, cols + half, leaf_dev * rank), BF16),
            pltpu.VMEM((leaf_dev, cols, points), F32),
            dma((6,)),
            dma((4 + wider,)),
            dma((10 + wider,)),
            dma((3,)),
            dma((3,)),
        ],
        compiler_params=pltpu.CompilerParams(
            collective_id=0, has_side_effects=True, vmem_limit_bytes=60 * 2**20
        ),
    )(panels, basis, transfer, near_blocks, coupling, near_list)


def solution(mesh):
    placed = (
        P("leaf", None, None),
        P("leaf", None, None),
        P("leaf", None, None),
        P("leaf", None, None, None),
        P(),
        P("leaf", None),
    )
    return jax.shard_map(
        per_device, mesh=mesh, in_specs=placed, out_specs=P("leaf", None, None), check_vma=False
    )
```

```python
import functools

import jax
import jax.numpy as jnp
from jax import lax
from jax.experimental import pallas as pl
from jax.experimental.pallas import tpu as pltpu
from jax.sharding import PartitionSpec as P

MESH = pl.DeviceIdType.MESH
F32 = jnp.float32
BF16 = jnp.bfloat16
REACH = 3
SPAN = 2 * REACH + 1
TN = (((0,), (0,)), ((), ()))
NT = (((1,), (1,)), ((), ()))
COEFS, PAIR, SUMS = range(3)


def axis_bits(first, bit_count):
    return [[b for b in range(bit_count) if (b + first) % 3 == a] for a in range(3)]


def halved(index, times):
    return index // 2**times if isinstance(index, int) else lax.div(index, 2**times)


def bit_of(index, b):
    high = halved(index, b) if b else index
    return high % 2 if isinstance(index, int) else lax.rem(high, 2)


def coords_of(index, bits):
    return [
        sum(bit_of(index, b) * 2**p for p, b in enumerate(bits[a])) + index * 0 for a in range(3)
    ]


def index_of(coords, bits):
    return sum(bit_of(coords[a], p) * 2**b for a in range(3) for p, b in enumerate(bits[a]))


def inside(coords, bits):
    ok = None
    for a in range(3):
        here = (coords[a] >= 0) & (coords[a] < 2 ** len(bits[a]))
        ok = here if ok is None else ok & here
    return ok


def flipped(index, mask, bit_count):
    result = 0
    for b in range(bit_count):
        one, two = bit_of(index, b), bit_of(mask, b)
        result = result + (one + two - 2 * one * two) * 2**b
    return result


def extract(coupling, code, level, spread, at):
    half = coupling.shape[1] // 2
    spread[at : at + 2 * half, :] = coupling[code].astype(F32)
    return spread[pl.ds(at + level, half, stride=2), :].astype(BF16)


def code_of(d):
    return (SPAN * (d[0] + REACH) + d[1] + REACH) * SPAN + d[2] + REACH


def kernel(
    n,
    panels_hbm,
    basis_hbm,
    transfer_hbm,
    blocks_hbm,
    coupling_hbm,
    near_hbm,
    out,
    panels,
    basis,
    transfer,
    blocks,
    coupling,
    near_list,
    slot_of,
    spread,
    mats0,
    mats1,
    coefs,
    reach,
    kept,
    pair_sent,
    pair_in,
    sent,
    sums,
    near,
    load_sem,
    panel_send,
    panel_recv,
    group_send,
    group_recv,
):
    leaf_dev, rank, points = basis.shape
    cols = panels.shape[1]
    slots = near_list.shape[1]
    shifts = coupling_hbm.shape[0]
    half = rank // 2
    low_bits = leaf_dev.bit_length() - 1
    dev_bits = n.bit_length() - 1
    bit_count = low_bits + dev_bits
    group = 8 // leaf_dev
    plane = min(8, n)
    plane_bits = plane.bit_length() - 1
    lines = n // plane
    teams = plane // group
    own_rows = (leaf_dev + 1) * half
    me = lax.axis_index("leaf")
    line, spot = lax.div(me, plane), lax.rem(me, plane)

    loads = [
        pltpu.make_async_copy(source, target, load_sem.at[i])
        for i, (source, target) in enumerate(
            [
                (panels_hbm, panels.at[pl.ds(me * leaf_dev, leaf_dev)]),
                (basis_hbm, basis),
                (transfer_hbm, transfer),
                (near_hbm, near_list),
                (coupling_hbm, coupling.at[pl.ds(0, shifts)]),
                (blocks_hbm, blocks),
            ]
        )
    ]
    for load in loads[:5]:
        load.start()

    bits = axis_bits(low_bits, dev_bits)
    where = coords_of(me, bits)
    side = [1 - 2 * bit_of(c, 0) for c in where]
    kinds = [min(2 ** len(b), 3) for b in bits]

    def offset(a, kind):
        return side[a] * bit_of(kind, 0) - side[a] * halved(kind, 1)

    def moved(kind):
        there = [where[a] + offset(a, kind[a]) for a in range(3)]
        ok = inside(there, bits)
        return ok, jnp.where(ok, index_of([jnp.maximum(v, 0) for v in there], bits), me)

    def when(kind, ok, act):
        if all(k < 2 for k in kind):
            act()
        else:
            pl.when(ok)(act)

    def peer(r):
        return line * plane + flipped(spot, r, plane_bits)

    barrier = pltpu.get_barrier_semaphore()

    def greet(device):
        pl.semaphore_signal(barrier, inc=1, device_id=(device,), device_id_type=MESH)

    @pl.loop(1, lines)
    def _(j):
        greet(lax.rem(line + j, lines) * plane + spot)

    for r in range(1, plane):
        greet(peer(r))
    faces = [tuple(k if b == a else 0 for b in range(3)) for a in range(3) for k in range(1, kinds[a])]
    expected = lines - 1 + plane - 1
    for face in faces:
        ok, to = moved(face)
        when(face, ok, lambda: greet(to))
        expected = expected + jnp.where(ok, 1, 0)

    coupling[shifts] = jnp.zeros((rank, 2 * rank), BF16)

    for load in loads[:3]:
        load.wait()
    lane = lax.broadcasted_iota(jnp.int32, (half, 2 * cols), 1)

    def packed(value, at):
        spread[at : at + rank, :] = value
        even = spread[pl.ds(at, half, stride=2), :]
        odd = spread[pl.ds(at + 1, half, stride=2), :]
        return jnp.where(lane < cols, even, odd).astype(BF16)

    def own_part(l):
        return pl.ds(pl.multiple_of((line * (leaf_dev + 1) + l) * half, half), half)

    flats = []
    for l in range(leaf_dev):
        panel = panels[me * leaf_dev + l]
        flat = lax.dot_general(
            basis[l], jnp.concatenate([panel, panel], axis=0), NT, preferred_element_type=F32
        )
        coefs[own_part(l), :] = packed(flat, l * rank)
        flats.append(flat.astype(BF16))
    term = None
    for l in range(leaf_dev):
        part = lax.dot_general(transfer[l], flats[l], TN, preferred_element_type=F32)
        term = part if term is None else term + part
    coefs[own_part(leaf_dev), :] = packed(term, leaf_dev * rank)

    along_x, along_y, along_z = (range(1, k) for k in kinds)

    def search():
        loads[3].wait()

        @pl.loop(0, kinds[1] * kinds[2])
        def _(i):
            y, z = lax.div(i, kinds[2]), lax.rem(i, kinds[2])

            def find(l, leaf):
                total = 0
                for k in range(slots):
                    total = jnp.where(near_list[l, k] == leaf, k, total)
                return total

            _, device = moved((0, y, z))
            for l in range(leaf_dev):
                for m in range(leaf_dev):
                    slot_of[i, l * leaf_dev + m] = find(l, device * leaf_dev + m)
            for x in along_x:
                e = offset(0, x)
                _, device = moved((x, y, z))
                leaf = device * leaf_dev + halved(1 - e, 1)
                slot_of[i, leaf_dev * leaf_dev + x - 1] = find(halved(1 + e, 1), leaf)

    early = line * 2 < lines
    pl.when(early)(search)

    pl.semaphore_wait(barrier, expected)

    def line_copy(j):
        block = coefs.at[pl.ds(pl.multiple_of(line * own_rows, own_rows), own_rows), :]
        return pltpu.make_async_remote_copy(
            src_ref=block,
            dst_ref=block,
            send_sem=group_send.at[COEFS],
            recv_sem=group_recv.at[COEFS],
            device_id=(j * plane + spot,),
            device_id_type=MESH,
        )

    def plane_copy(r, source, target, which):
        return pltpu.make_async_remote_copy(
            src_ref=source,
            dst_ref=target,
            send_sem=group_send.at[which],
            recv_sem=group_recv.at[which],
            device_id=(peer(r),),
            device_id_type=MESH,
        )

    def everything(which):
        whole = {
            COEFS: coefs.at[pl.ds(0, (lines - 1) * own_rows), :],
            PAIR: pair_in,
            SUMS: sums,
        }[which]
        return plane_copy(1, whole, whole, which)

    front = halved(1 + side[0], 1)

    def semaphores(kind, late=0):
        far = [int(k > 1) for k in kind]
        if far[0]:
            at = kind[1] * kinds[2] + kind[2]
            return 4 + at, 10 + at
        if kind[1]:
            at = 4 + kind[1] + 2 * far[2]
        elif kind[0]:
            at = (1, 2, 9)[kind[2]]
        else:
            at = (0, 0, 3 + late)[kind[2]]
        return 2 * far[1] + far[2], at

    def panel_copy(kind, lane, source, receiver):
        first, count, late = 0, leaf_dev, 0
        if kind[0]:
            first, count = lane, 1
        elif lane is not None:
            first, count, late = (front, 1 - front)[lane], 1, lane
        rows = panels.at[pl.ds(source * leaf_dev + first, count)]
        from_at, to_at = semaphores(kind, late)
        return pltpu.make_async_remote_copy(
            src_ref=rows,
            dst_ref=rows,
            send_sem=panel_send.at[from_at],
            recv_sem=panel_recv.at[to_at],
            device_id=(receiver,),
            device_id_type=MESH,
        )

    def lanes_of(kind):
        return (0, 1) if kind[0] == 0 and kind[2] > 1 else (None,)

    def hops_of(kind):
        if kind[0] and kind[1] and (kind[1] > 1 or kind[2] > 1) and kind[2]:
            return (kind[0], kind[1], 0)
        a = 1 if kind[1] else 0 if kind[0] else 2
        return tuple(k if b == a else 0 for b, k in enumerate(kind))

    def sends(kind, act, lane=None):
        hop = hops_of(kind)
        rest = tuple(k - h for k, h in zip(kind, hop))
        ok, to = moved(hop)
        known, source = moved(rest)
        if kind[0]:
            lane = halved(1 + offset(0, kind[0]) * (1 if hop[0] else -1), 1)
        when(kind, ok & known, lambda: act(panel_copy(kind, lane, source, to)))

    def whole(count, from_at, to_at):
        rows = panels.at[pl.ds(0, count)]
        return pltpu.make_async_remote_copy(
            src_ref=rows,
            dst_ref=rows,
            send_sem=panel_send.at[from_at],
            recv_sem=panel_recv.at[to_at],
            device_id=(peer(1),),
            device_id_type=MESH,
        )

    def arrived(members, lane=None):
        count = 0
        for kind in members:
            if kind[0] > 1:
                single = whole(1, *semaphores(kind))
                when(kind, moved(kind)[0], lambda: single.wait_recv())
            else:
                count += leaf_dev if kind[0] == 0 and lane is None else 1
                from_at, to_at = semaphores(kind, lane or 0)
                last = kind
        if count:
            copy = whole(count, from_at, to_at)
            when(last, moved(last)[0], lambda: copy.wait_recv())

    def start(copy):
        copy.start()

    def gather(first, last):
        @pl.loop(first, last)
        def _(j):
            @pl.when(j != line)
            def _():
                line_copy(j).start()

    gather(0, max(lines // 4, 1))
    if kinds[2] > 2:
        sends((0, 0, 2), start, 0)
    gather(max(lines // 4, 1), lines)

    if kinds[2] > 2:
        sends((0, 0, 2), start, 1)
    sends((0, 0, 1), start)
    for x in along_x:
        sends((x, 0, 0), start)
    for y in reversed(along_y):
        sends((0, y, 0), start)

    loads[4].wait()
    loads[5].start()

    chunk = min(8 // leaf_dev, lines)
    chunks = lines // chunk
    parents = bit_count - 3
    parent_bits = axis_bits(0, parents)
    team = lax.div(spot, group)

    def parent_mats(c):
        for t in range(teams):
            goal = line * teams + flipped(team, t, teams.bit_length() - 1)
            target = coords_of(goal, parent_bits)
            for j in range(chunk):
                source = coords_of((c * chunk + j) * teams + team, parent_bits)
                d = [source[a] - target[a] for a in range(3)]
                use = (jnp.abs(d[0]) > 1) | (jnp.abs(d[1]) > 1) | (jnp.abs(d[2]) > 1)
                for a in range(3):
                    use = use & (jnp.abs(halved(source[a], 1) - halved(target[a], 1)) <= 1)
                code = jnp.where(use, code_of(d), shifts)
                mat = extract(coupling, code, 1, spread, (t * chunk + j) * rank)
                rows = slice(j * half, (j + 1) * half)
                mats1[c, rows, 2 * rank * t : 2 * rank * (t + 1)] = mat

    here = coords_of(line * plane, bits)
    base = coords_of(spot, bits)

    def leaf_mats(c):
        for r in range(plane):
            goal = list(base)
            for a in range(3):
                for p, b in enumerate(bits[a]):
                    if b < plane_bits and r >> b & 1:
                        goal[a] = goal[a] + (1 - 2 * bit_of(spot, b)) * 2**p
            target = [here[a] + goal[a] for a in range(3)]
            for j in range(chunk):
                there = coords_of((c * chunk + j) * plane, bits)
                source = [there[a] + base[a] for a in range(3)]
                d = [source[a] - target[a] for a in range(3)]
                close = jnp.abs(d[0]) <= 1
                for a in (1, 2):
                    close = close & (jnp.abs(halved(source[a], 1) - halved(target[a], 1)) <= 1)
                apart = (jnp.abs(d[1]) > 1) | (jnp.abs(d[2]) > 1)
                parts = {}
                for e in range(1 - leaf_dev, leaf_dev):
                    dx = leaf_dev * d[0] + e
                    use = close & (apart | (jnp.abs(dx) > 1))
                    code = jnp.where(use, code_of([dx, d[1], d[2]]), shifts)
                    at = ((r % 2 * chunk + j) * (2 * leaf_dev - 1) + e + leaf_dev - 1) * rank
                    parts[e] = extract(coupling, code, 0, spread, at)
                for m in range(leaf_dev):
                    rows = slice((j * leaf_dev + m) * half, (j * leaf_dev + m + 1) * half)
                    for l in range(leaf_dev):
                        mats0[c * plane + r, rows, 2 * rank * l : 2 * rank * (l + 1)] = parts[m - l]

    for build in (parent_mats, leaf_mats):
        if chunks == 1:
            build(0)
        else:
            pl.loop(0, chunks)(build)

    reach[: leaf_dev * rank] = basis[...].reshape(leaf_dev * rank, points)
    for l in range(leaf_dev):
        lift = lax.dot_general(transfer[l], basis[l], TN, preferred_element_type=F32).astype(BF16)
        for p in range(2):
            at = (leaf_dev + 2 * l + p) * rank
            reach[at : at + rank] = lift

    for x in along_x:
        arrived([(x, 0, 0)])
        for y in reversed(along_y):
            sends((x, y, 0), start)
    arrived([(0, 0, 1)])
    for x in along_x:
        sends((x, 0, 1), start)
        if kinds[1] > 2:
            sends((x, 2, 1), start)
    for y in reversed(along_y):
        sends((0, y, 1), start)

    hurried = (line * 4 < lines) & (lax.rem(spot, 2) == 0)

    def relay(lane):
        arrived([(0, 0, 2)], lane)
        x = 1 + lane
        if x in along_x:
            sends((x, 0, 2), start)
            for y in reversed(along_y):
                sends((x, y, 2), start)
        for y in reversed(along_y):
            sends((0, y, 2), start, lane)

    everything(COEFS).wait_recv()
    wide = lax.broadcasted_iota(jnp.int32, (cols, 2 * rank), 1) < rank
    def gathered(c, first, count):
        parts = []
        for j in range(chunk):
            at = (c * chunk + j) * own_rows + first * half
            parts.append(coefs[at : at + count * half, :])
        return jnp.concatenate(parts, axis=0)

    def applied(first, count, mats, at):
        total = None
        for c in range(chunks):
            part = lax.dot_general(
                gathered(c, first, count), mats[c * at[1] + at[0]], TN, preferred_element_type=F32
            )
            total = part if total is None else total + part
        return total

    low = lax.broadcasted_iota(jnp.int32, (half, 2 * rank), 1) < rank
    every_down = applied(leaf_dev, 1, mats1, (0, 1))
    downs = []
    for t in range(teams):
        one = every_down[:, 2 * rank * t : 2 * rank * (t + 1)]
        straight = jnp.where(low, one[:half], one[cols + half :])
        crossed = jnp.where(low, one[half:cols], one[cols : cols + half])
        downs.append(straight + pltpu.roll(crossed, rank, 1))

    def partial(r):
        total = applied(0, leaf_dev, mats0, (r, plane))
        one, two = total[:, : 2 * rank], total[:, 2 * rank :]
        straight = jnp.where(wide, one[:cols], two[cols:])
        crossed = jnp.where(wide, two[:cols], one[cols:])
        return straight + pltpu.roll(crossed, rank, 1), downs[r // group]

    for i in range(plane // 2):
        result, down = partial(2 * i + 1)
        pair_sent[i, :cols] = result.astype(BF16)
        pair_sent[i, cols:] = down.astype(BF16)
    plane_copy(1, pair_sent, pair_in, PAIR).start()
    for i in range(plane // 2):
        result, down = partial(2 * i)
        kept[i, :cols] = result
        kept[i, cols:] = down
    if kinds[2] > 2:
        pl.when(~hurried)(lambda: relay(0))
    everything(PAIR).wait_recv()
    for i in reversed(range(1, plane // 2)):
        sent[i - 1] = (kept[i] + pair_in[i].astype(F32)).astype(BF16)
    for i in reversed(range(1, plane // 2)):
        plane_copy(2 * i, sent.at[i - 1], sums.at[i - 1], SUMS).start()

    if kinds[2] > 2:
        pl.when(hurried)(lambda: relay(0))
        relay(1)

    for x in along_x:
        arrived([(x, 0, 1)])
        sends((x, 1, 1), start)

    def near_part(y, levels, first=False):
        totals = [None] * leaf_dev
        outer = [None] * len(along_x)

        def add(old, panel, l, slot):
            part = jnp.dot(panel, blocks[l, slot], preferred_element_type=F32)
            return part if old is None else old + part

        for z in levels:
            at = y * kinds[2] + z
            _, device = moved((0, y, z))
            for m in range(leaf_dev):
                panel = panels[device * leaf_dev + m]
                for l in range(leaf_dev):
                    totals[l] = add(totals[l], panel, l, slot_of[at, l * leaf_dev + m])
            for x in along_x:
                e = offset(0, x)
                ok, device = moved((x, y, z))
                panel = panels[device * leaf_dev + halved(1 - e, 1)]
                if x > 1:
                    panel = jnp.where(ok, panel, jnp.zeros_like(panel))
                slot = slot_of[at, leaf_dev * leaf_dev + x - 1]
                outer[x - 1] = add(outer[x - 1], panel, halved(1 + e, 1), slot)
        for l in range(leaf_dev):
            near[l] = totals[l] if first else near[l] + totals[l]
        for x in along_x:
            l = halved(1 + offset(0, x), 1)
            near[l] = near[l] + outer[x - 1]

    def near_when(y, levels):
        if y:
            arrived([(x, y, z) for x in range(kinds[0]) for z in levels])
        kind = (0, y, max(levels))
        when(kind, moved(kind)[0], lambda: near_part(y, levels))

    pl.when(~early)(search)
    loads[5].wait()
    near_part(0, range(2), first=True)
    for y in reversed(along_y):
        near_when(y, range(2))
    if kinds[2] > 2:
        for x in along_x:
            arrived([(x, 0, 2)])
        near_when(0, [2])
        near_when(1, [2])

    if kinds[1] > 2 and kinds[2] > 2:
        near_when(2, [2])

    every = [
        (x, y, z)
        for x in range(kinds[0])
        for y in range(kinds[1])
        for z in range(kinds[2])
        if x or y or z
    ]
    for y in range(kinds[1] - 1):
        for z in range(kinds[2] - 1):
            mine = [k for k in every if k[0] < 2 and (k[1] > 1) == y and (k[2] > 1) == z]
            last = mine[-1]
            count = sum(1 if k[0] else leaf_dev for k in mine)
            copy = whole(count, *semaphores(last))
            when(last, moved((0,) + last[1:])[0], lambda: copy.wait_send())
    for kind in every:
        if kind[0] > 1:
            sends(kind, lambda copy: copy.wait_send())
    everything(COEFS).wait_send()
    everything(PAIR).wait_send()

    everything(SUMS).wait_recv()
    total = kept[0] + pair_in[0].astype(F32)
    for i in range(plane // 2 - 1):
        total = total + sums[i].astype(F32)
    leafs, down = total[:cols], total[cols:]
    none = jnp.zeros_like(leafs)
    down = jnp.concatenate([jnp.where(low, down, 0.0), jnp.where(low, 0.0, down)], axis=0)
    pair = jnp.concatenate(
        [
            jnp.concatenate([jnp.where(wide, leafs, 0.0), jnp.where(wide, 0.0, leafs)], axis=0),
            jnp.concatenate([down, none], axis=0),
            jnp.concatenate([none, down], axis=0),
        ],
        axis=1,
    )
    far = jnp.dot(pair.astype(BF16), reach[...], preferred_element_type=F32)
    for l in range(leaf_dev):
        out[l] = (near[l] + far[l * cols : (l + 1) * cols]).astype(BF16)
    everything(SUMS).wait_send()


def per_device(panels, basis, transfer, near_blocks, coupling, near_list):
    n = lax.axis_size("leaf")
    leaf_dev, cols, points = panels.shape
    rank = basis.shape[1]
    slots = near_list.shape[1]
    shifts = coupling.shape[1]
    half = rank // 2
    leaves = n * leaf_dev
    coupling = coupling.transpose(1, 0, 2).reshape(shifts, 2, half, 2 * rank)
    coupling = coupling.transpose(0, 2, 1, 3).reshape(shifts, rank, 2 * rank)
    plane = min(8, n)
    lines = n // plane
    teams = plane * leaf_dev // 8
    chunk = min(8 // leaf_dev, lines)
    kinds = [min(2 ** len(b), 3) for b in axis_bits(leaf_dev.bit_length() - 1, n.bit_length() - 1)]
    wider = kinds[1] * kinds[2] if kinds[0] > 2 else 0
    dma = pltpu.SemaphoreType.DMA
    return pl.pallas_call(
        functools.partial(kernel, n),
        out_shape=pltpu.VMEM(panels.shape, BF16),
        in_specs=[pl.BlockSpec(memory_space=pl.ANY)] * 6,
        out_specs=pl.BlockSpec(memory_space=pltpu.VMEM),
        scratch_shapes=[
            pltpu.VMEM((leaves, cols, points), BF16),
            pltpu.VMEM(basis.shape, BF16),
            pltpu.VMEM(transfer.shape, BF16),
            pltpu.VMEM(near_blocks.shape, BF16),
            pltpu.VMEM((shifts + 1, rank, 2 * rank), BF16),
            pltpu.SMEM(near_list.shape, jnp.int32),
            pltpu.SMEM((kinds[1] * kinds[2], leaf_dev * leaf_dev + 2), jnp.int32),
            pltpu.VMEM((max(2 * chunk * (2 * leaf_dev - 1), 8) * rank, 2 * rank), F32),
            pltpu.VMEM(
                (plane * (lines // chunk), chunk * leaf_dev * half, 2 * rank * leaf_dev), BF16
            ),
            pltpu.VMEM((lines // chunk, chunk * half, 2 * rank * teams), BF16),
            pltpu.VMEM((lines * (leaf_dev + 1) * half, 2 * cols), BF16),
            pltpu.VMEM((3 * leaf_dev * rank, points), BF16),
            pltpu.VMEM((plane // 2, cols + half, leaf_dev * rank), F32),
            pltpu.VMEM((plane // 2, cols + half, leaf_dev * rank), BF16),
            pltpu.VMEM((plane // 2, cols + half, leaf_dev * rank), BF16),
            pltpu.VMEM((plane // 2 - 1, cols + half, leaf_dev * rank), BF16),
            pltpu.VMEM((plane // 2 - 1, cols + half, leaf_dev * rank), BF16),
            pltpu.VMEM((leaf_dev, cols, points), F32),
            dma((6,)),
            dma((4 + wider,)),
            dma((10 + wider,)),
            dma((3,)),
            dma((3,)),
        ],
        compiler_params=pltpu.CompilerParams(
            collective_id=0, has_side_effects=True, vmem_limit_bytes=60 * 2**20
        ),
    )(panels, basis, transfer, near_blocks, coupling, near_list)


def solution(mesh):
    placed = (
        P("leaf", None, None),
        P("leaf", None, None),
        P("leaf", None, None),
        P("leaf", None, None, None),
        P(),
        P("leaf", None),
    )
    return jax.shard_map(
        per_device, mesh=mesh, in_specs=placed, out_specs=P("leaf", None, None), check_vma=False
    )
```

```python
import functools

import jax
import jax.numpy as jnp
from jax import lax
from jax.experimental import pallas as pl
from jax.experimental.pallas import tpu as pltpu
from jax.sharding import PartitionSpec as P

MESH = pl.DeviceIdType.MESH
F32 = jnp.float32
BF16 = jnp.bfloat16
REACH = 3
SPAN = 2 * REACH + 1
TN = (((0,), (0,)), ((), ()))
NT = (((1,), (1,)), ((), ()))
COEFS, PAIR, SUMS = range(3)


def axis_bits(first, bit_count):
    return [[b for b in range(bit_count) if (b + first) % 3 == a] for a in range(3)]


def halved(index, times):
    return index // 2**times if isinstance(index, int) else lax.div(index, 2**times)


def bit_of(index, b):
    high = halved(index, b) if b else index
    return high % 2 if isinstance(index, int) else lax.rem(high, 2)


def coords_of(index, bits):
    return [
        sum(bit_of(index, b) * 2**p for p, b in enumerate(bits[a])) + index * 0 for a in range(3)
    ]


def index_of(coords, bits):
    return sum(bit_of(coords[a], p) * 2**b for a in range(3) for p, b in enumerate(bits[a]))


def inside(coords, bits):
    ok = None
    for a in range(3):
        here = (coords[a] >= 0) & (coords[a] < 2 ** len(bits[a]))
        ok = here if ok is None else ok & here
    return ok


def flipped(index, mask, bit_count):
    result = 0
    for b in range(bit_count):
        one, two = bit_of(index, b), bit_of(mask, b)
        result = result + (one + two - 2 * one * two) * 2**b
    return result


def extract(coupling, code, level, spread, at):
    half = coupling.shape[1] // 2
    spread[at : at + 2 * half, :] = coupling[code].astype(F32)
    return spread[pl.ds(at + level, half, stride=2), :].astype(BF16)


def code_of(d):
    return (SPAN * (d[0] + REACH) + d[1] + REACH) * SPAN + d[2] + REACH


def kernel(
    n,
    panels_hbm,
    basis_hbm,
    transfer_hbm,
    blocks_hbm,
    coupling_hbm,
    near_hbm,
    out,
    panels,
    basis,
    transfer,
    blocks,
    coupling,
    near_list,
    slot_of,
    spread,
    mats0,
    mats1,
    coefs,
    reach,
    kept,
    pair_sent,
    pair_in,
    sent,
    sums,
    near,
    load_sem,
    panel_send,
    panel_recv,
    group_send,
    group_recv,
):
    leaf_dev, rank, points = basis.shape
    cols = panels.shape[1]
    slots = near_list.shape[1]
    shifts = coupling_hbm.shape[0]
    half = rank // 2
    low_bits = leaf_dev.bit_length() - 1
    dev_bits = n.bit_length() - 1
    bit_count = low_bits + dev_bits
    group = 8 // leaf_dev
    plane = min(8, n)
    plane_bits = plane.bit_length() - 1
    lines = n // plane
    teams = plane // group
    own_rows = (leaf_dev + 1) * half
    me = lax.axis_index("leaf")
    line, spot = lax.div(me, plane), lax.rem(me, plane)

    loads = [
        pltpu.make_async_copy(source, target, load_sem.at[i])
        for i, (source, target) in enumerate(
            [
                (panels_hbm, panels.at[pl.ds(me * leaf_dev, leaf_dev)]),
                (basis_hbm, basis),
                (transfer_hbm, transfer),
                (near_hbm, near_list),
                (coupling_hbm, coupling.at[pl.ds(0, shifts)]),
                (blocks_hbm, blocks),
            ]
        )
    ]
    for load in loads[:5]:
        load.start()

    bits = axis_bits(low_bits, dev_bits)
    where = coords_of(me, bits)
    side = [1 - 2 * bit_of(c, 0) for c in where]
    kinds = [min(2 ** len(b), 3) for b in bits]

    def offset(a, kind):
        return side[a] * bit_of(kind, 0) - side[a] * halved(kind, 1)

    def moved(kind):
        there = [where[a] + offset(a, kind[a]) for a in range(3)]
        ok = inside(there, bits)
        return ok, jnp.where(ok, index_of([jnp.maximum(v, 0) for v in there], bits), me)

    def when(kind, ok, act):
        if all(k < 2 for k in kind):
            act()
        else:
            pl.when(ok)(act)

    def peer(r):
        return line * plane + flipped(spot, r, plane_bits)

    barrier = pltpu.get_barrier_semaphore()

    def greet(device):
        pl.semaphore_signal(barrier, inc=1, device_id=(device,), device_id_type=MESH)

    @pl.loop(1, lines)
    def _(j):
        greet(lax.rem(line + j, lines) * plane + spot)

    for r in range(1, plane):
        greet(peer(r))
    faces = [tuple(k if b == a else 0 for b in range(3)) for a in range(3) for k in range(1, kinds[a])]
    expected = lines - 1 + plane - 1
    for face in faces:
        ok, to = moved(face)
        when(face, ok, lambda: greet(to))
        expected = expected + jnp.where(ok, 1, 0)

    coupling[shifts] = jnp.zeros((rank, 2 * rank), BF16)

    for load in loads[:3]:
        load.wait()
    lane = lax.broadcasted_iota(jnp.int32, (half, 2 * cols), 1)

    def packed(value, at):
        spread[at : at + rank, :] = value
        even = spread[pl.ds(at, half, stride=2), :]
        odd = spread[pl.ds(at + 1, half, stride=2), :]
        return jnp.where(lane < cols, even, odd).astype(BF16)

    def own_part(l):
        return pl.ds(pl.multiple_of((line * (leaf_dev + 1) + l) * half, half), half)

    flats = []
    for l in range(leaf_dev):
        panel = panels[me * leaf_dev + l]
        flat = lax.dot_general(
            basis[l], jnp.concatenate([panel, panel], axis=0), NT, preferred_element_type=F32
        )
        coefs[own_part(l), :] = packed(flat, l * rank)
        flats.append(flat.astype(BF16))
    term = None
    for l in range(leaf_dev):
        part = lax.dot_general(transfer[l], flats[l], TN, preferred_element_type=F32)
        term = part if term is None else term + part
    coefs[own_part(leaf_dev), :] = packed(term, leaf_dev * rank)

    along_x, along_y, along_z = (range(1, k) for k in kinds)

    def search():
        loads[3].wait()

        @pl.loop(0, kinds[1] * kinds[2])
        def _(i):
            y, z = lax.div(i, kinds[2]), lax.rem(i, kinds[2])

            def find(l, leaf):
                total = 0
                for k in range(slots):
                    total = jnp.where(near_list[l, k] == leaf, k, total)
                return total

            _, device = moved((0, y, z))
            for l in range(leaf_dev):
                for m in range(leaf_dev):
                    slot_of[i, l * leaf_dev + m] = find(l, device * leaf_dev + m)
            for x in along_x:
                e = offset(0, x)
                _, device = moved((x, y, z))
                leaf = device * leaf_dev + halved(1 - e, 1)
                slot_of[i, leaf_dev * leaf_dev + x - 1] = find(halved(1 + e, 1), leaf)

    early = line * 2 < lines
    pl.when(early)(search)

    pl.semaphore_wait(barrier, expected)

    def line_copy(j):
        block = coefs.at[pl.ds(pl.multiple_of(line * own_rows, own_rows), own_rows), :]
        return pltpu.make_async_remote_copy(
            src_ref=block,
            dst_ref=block,
            send_sem=group_send.at[COEFS],
            recv_sem=group_recv.at[COEFS],
            device_id=(j * plane + spot,),
            device_id_type=MESH,
        )

    def plane_copy(r, source, target, which):
        return pltpu.make_async_remote_copy(
            src_ref=source,
            dst_ref=target,
            send_sem=group_send.at[which],
            recv_sem=group_recv.at[which],
            device_id=(peer(r),),
            device_id_type=MESH,
        )

    def everything(which):
        whole = {
            COEFS: coefs.at[pl.ds(0, (lines - 1) * own_rows), :],
            PAIR: pair_in,
            SUMS: sums,
        }[which]
        return plane_copy(1, whole, whole, which)

    front = halved(1 + side[0], 1)

    def semaphores(kind, late=0):
        far = [int(k > 1) for k in kind]
        if far[0]:
            at = kind[1] * kinds[2] + kind[2]
            return 4 + at, 10 + at
        if kind[1]:
            at = 4 + kind[1] + 2 * far[2]
        elif kind[0]:
            at = (1, 2, 9)[kind[2]]
        else:
            at = (0, 0, 3 + late)[kind[2]]
        return 2 * far[1] + far[2], at

    def panel_copy(kind, lane, source, receiver):
        first, count, late = 0, leaf_dev, 0
        if kind[0]:
            first, count = lane, 1
        elif lane is not None:
            first, count, late = (front, 1 - front)[lane], 1, lane
        rows = panels.at[pl.ds(source * leaf_dev + first, count)]
        from_at, to_at = semaphores(kind, late)
        return pltpu.make_async_remote_copy(
            src_ref=rows,
            dst_ref=rows,
            send_sem=panel_send.at[from_at],
            recv_sem=panel_recv.at[to_at],
            device_id=(receiver,),
            device_id_type=MESH,
        )

    def lanes_of(kind):
        return (0, 1) if kind[0] == 0 and kind[2] > 1 else (None,)

    def hops_of(kind):
        if kind[0] and kind[1] and (kind[1] > 1 or kind[2] > 1) and kind[2]:
            return (kind[0], kind[1], 0)
        a = 1 if kind[1] else 0 if kind[0] else 2
        return tuple(k if b == a else 0 for b, k in enumerate(kind))

    def sends(kind, act, lane=None):
        hop = hops_of(kind)
        rest = tuple(k - h for k, h in zip(kind, hop))
        ok, to = moved(hop)
        known, source = moved(rest)
        if kind[0]:
            lane = halved(1 + offset(0, kind[0]) * (1 if hop[0] else -1), 1)
        when(kind, ok & known, lambda: act(panel_copy(kind, lane, source, to)))

    def whole(count, from_at, to_at):
        rows = panels.at[pl.ds(0, count)]
        return pltpu.make_async_remote_copy(
            src_ref=rows,
            dst_ref=rows,
            send_sem=panel_send.at[from_at],
            recv_sem=panel_recv.at[to_at],
            device_id=(peer(1),),
            device_id_type=MESH,
        )

    def arrived(members, lane=None):
        count = 0
        for kind in members:
            if kind[0] > 1:
                single = whole(1, *semaphores(kind))
                when(kind, moved(kind)[0], lambda: single.wait_recv())
            else:
                count += leaf_dev if kind[0] == 0 and lane is None else 1
                from_at, to_at = semaphores(kind, lane or 0)
                last = kind
        if count:
            copy = whole(count, from_at, to_at)
            when(last, moved(last)[0], lambda: copy.wait_recv())

    def start(copy):
        copy.start()

    def gather(first, last):
        @pl.loop(first, last)
        def _(j):
            @pl.when(j != line)
            def _():
                line_copy(j).start()

    gather(0, max(lines // 4, 1))
    if kinds[2] > 2:
        sends((0, 0, 2), start, 0)
    gather(max(lines // 4, 1), lines)

    if kinds[2] > 2:
        sends((0, 0, 2), start, 1)
    sends((0, 0, 1), start)
    for x in along_x:
        sends((x, 0, 0), start)
    for y in reversed(along_y):
        sends((0, y, 0), start)

    loads[4].wait()
    loads[5].start()

    chunk = min(8 // leaf_dev, lines)
    chunks = lines // chunk
    parents = bit_count - 3
    parent_bits = axis_bits(0, parents)
    team = lax.div(spot, group)

    def parent_mats(c):
        for t in range(teams):
            goal = line * teams + flipped(team, t, teams.bit_length() - 1)
            target = coords_of(goal, parent_bits)
            for j in range(chunk):
                source = coords_of((c * chunk + j) * teams + team, parent_bits)
                d = [source[a] - target[a] for a in range(3)]
                use = (jnp.abs(d[0]) > 1) | (jnp.abs(d[1]) > 1) | (jnp.abs(d[2]) > 1)
                for a in range(3):
                    use = use & (jnp.abs(halved(source[a], 1) - halved(target[a], 1)) <= 1)
                code = jnp.where(use, code_of(d), shifts)
                mat = extract(coupling, code, 1, spread, (t * chunk + j) * rank)
                rows = slice(j * half, (j + 1) * half)
                mats1[c, rows, 2 * rank * t : 2 * rank * (t + 1)] = mat

    here = coords_of(line * plane, bits)
    base = coords_of(spot, bits)

    def leaf_mats(c):
        for r in range(plane):
            goal = list(base)
            for a in range(3):
                for p, b in enumerate(bits[a]):
                    if b < plane_bits and r >> b & 1:
                        goal[a] = goal[a] + (1 - 2 * bit_of(spot, b)) * 2**p
            target = [here[a] + goal[a] for a in range(3)]
            for j in range(chunk):
                there = coords_of((c * chunk + j) * plane, bits)
                source = [there[a] + base[a] for a in range(3)]
                d = [source[a] - target[a] for a in range(3)]
                close = jnp.abs(d[0]) <= 1
                for a in (1, 2):
                    close = close & (jnp.abs(halved(source[a], 1) - halved(target[a], 1)) <= 1)
                apart = (jnp.abs(d[1]) > 1) | (jnp.abs(d[2]) > 1)
                parts = {}
                for e in range(1 - leaf_dev, leaf_dev):
                    dx = leaf_dev * d[0] + e
                    use = close & (apart | (jnp.abs(dx) > 1))
                    code = jnp.where(use, code_of([dx, d[1], d[2]]), shifts)
                    at = ((r % 2 * chunk + j) * (2 * leaf_dev - 1) + e + leaf_dev - 1) * rank
                    parts[e] = extract(coupling, code, 0, spread, at)
                for m in range(leaf_dev):
                    rows = slice((j * leaf_dev + m) * half, (j * leaf_dev + m + 1) * half)
                    for l in range(leaf_dev):
                        mats0[c * plane + r, rows, 2 * rank * l : 2 * rank * (l + 1)] = parts[m - l]

    for build in (parent_mats, leaf_mats):
        if chunks == 1:
            build(0)
        else:
            pl.loop(0, chunks)(build)

    reach[: leaf_dev * rank] = basis[...].reshape(leaf_dev * rank, points)
    for l in range(leaf_dev):
        lift = lax.dot_general(transfer[l], basis[l], TN, preferred_element_type=F32).astype(BF16)
        for p in range(2):
            at = (leaf_dev + 2 * l + p) * rank
            reach[at : at + rank] = lift

    for x in along_x:
        arrived([(x, 0, 0)])
        for y in reversed(along_y):
            sends((x, y, 0), start)
    arrived([(0, 0, 1)])
    for x in along_x:
        sends((x, 0, 1), start)
        if kinds[1] > 2:
            sends((x, 2, 1), start)
    for y in reversed(along_y):
        sends((0, y, 1), start)

    hurried = (line * 4 < lines) & (lax.rem(spot, 2) == 0)

    def relay(lane):
        arrived([(0, 0, 2)], lane)
        x = 1 + lane
        if x in along_x:
            sends((x, 0, 2), start)
            for y in reversed(along_y):
                sends((x, y, 2), start)
        for y in reversed(along_y):
            sends((0, y, 2), start, lane)

    everything(COEFS).wait_recv()
    wide = lax.broadcasted_iota(jnp.int32, (cols, 2 * rank), 1) < rank
    def gathered(c, first, count):
        parts = []
        for j in range(chunk):
            at = (c * chunk + j) * own_rows + first * half
            parts.append(coefs[at : at + count * half, :])
        return jnp.concatenate(parts, axis=0)

    def applied(first, count, mats, at):
        total = None
        for c in range(chunks):
            part = lax.dot_general(
                gathered(c, first, count), mats[c * at[1] + at[0]], TN, preferred_element_type=F32
            )
            total = part if total is None else total + part
        return total

    low = lax.broadcasted_iota(jnp.int32, (half, 2 * rank), 1) < rank
    every_down = applied(leaf_dev, 1, mats1, (0, 1))
    downs = []
    for t in range(teams):
        one = every_down[:, 2 * rank * t : 2 * rank * (t + 1)]
        straight = jnp.where(low, one[:half], one[cols + half :])
        crossed = jnp.where(low, one[half:cols], one[cols : cols + half])
        downs.append(straight + pltpu.roll(crossed, rank, 1))

    def partial(r):
        total = applied(0, leaf_dev, mats0, (r, plane))
        one, two = total[:, : 2 * rank], total[:, 2 * rank :]
        straight = jnp.where(wide, one[:cols], two[cols:])
        crossed = jnp.where(wide, two[:cols], one[cols:])
        return straight + pltpu.roll(crossed, rank, 1), downs[r // group]

    for i in range(plane // 2):
        result, down = partial(2 * i + 1)
        pair_sent[i, :cols] = result.astype(BF16)
        pair_sent[i, cols:] = down.astype(BF16)
    plane_copy(1, pair_sent, pair_in, PAIR).start()
    for i in range(plane // 2):
        result, down = partial(2 * i)
        kept[i, :cols] = result
        kept[i, cols:] = down
    if kinds[2] > 2:
        pl.when(~hurried)(lambda: relay(0))
    everything(PAIR).wait_recv()
    for i in reversed(range(1, plane // 2)):
        sent[i - 1] = (kept[i] + pair_in[i].astype(F32)).astype(BF16)
    for i in reversed(range(1, plane // 2)):
        plane_copy(2 * i, sent.at[i - 1], sums.at[i - 1], SUMS).start()

    if kinds[2] > 2:
        pl.when(hurried)(lambda: relay(0))
        relay(1)

    for x in along_x:
        arrived([(x, 0, 1)])
        sends((x, 1, 1), start)

    def near_part(y, levels, first=False):
        totals = [None] * leaf_dev
        outer = [None] * len(along_x)

        def add(old, panel, l, slot):
            part = jnp.dot(panel, blocks[l, slot], preferred_element_type=F32)
            return part if old is None else old + part

        for z in levels:
            at = y * kinds[2] + z
            _, device = moved((0, y, z))
            for m in range(leaf_dev):
                panel = panels[device * leaf_dev + m]
                for l in range(leaf_dev):
                    totals[l] = add(totals[l], panel, l, slot_of[at, l * leaf_dev + m])
            for x in along_x:
                e = offset(0, x)
                ok, device = moved((x, y, z))
                panel = panels[device * leaf_dev + halved(1 - e, 1)]
                if x > 1:
                    panel = jnp.where(ok, panel, jnp.zeros_like(panel))
                slot = slot_of[at, leaf_dev * leaf_dev + x - 1]
                outer[x - 1] = add(outer[x - 1], panel, halved(1 + e, 1), slot)
        for l in range(leaf_dev):
            near[l] = totals[l] if first else near[l] + totals[l]
        for x in along_x:
            l = halved(1 + offset(0, x), 1)
            near[l] = near[l] + outer[x - 1]

    def near_when(y, levels):
        if y:
            arrived([(x, y, z) for x in range(kinds[0]) for z in levels])
        kind = (0, y, max(levels))
        when(kind, moved(kind)[0], lambda: near_part(y, levels))

    pl.when(~early)(search)
    loads[5].wait()
    near_part(0, range(2), first=True)
    for y in reversed(along_y):
        near_when(y, range(2))
    if kinds[2] > 2:
        for x in along_x:
            arrived([(x, 0, 2)])
        near_when(0, [2])
        if kinds[1] > 2:
            near_when(2, [2])
        near_when(1, [2])

    every = [
        (x, y, z)
        for x in range(kinds[0])
        for y in range(kinds[1])
        for z in range(kinds[2])
        if x or y or z
    ]
    for y in range(kinds[1] - 1):
        for z in range(kinds[2] - 1):
            mine = [k for k in every if k[0] < 2 and (k[1] > 1) == y and (k[2] > 1) == z]
            last = mine[-1]
            count = sum(1 if k[0] else leaf_dev for k in mine)
            copy = whole(count, *semaphores(last))
            when(last, moved((0,) + last[1:])[0], lambda: copy.wait_send())
    for kind in every:
        if kind[0] > 1:
            sends(kind, lambda copy: copy.wait_send())
    everything(COEFS).wait_send()
    everything(PAIR).wait_send()

    everything(SUMS).wait_recv()
    total = kept[0] + pair_in[0].astype(F32)
    for i in range(plane // 2 - 1):
        total = total + sums[i].astype(F32)
    leafs, down = total[:cols], total[cols:]
    none = jnp.zeros_like(leafs)
    down = jnp.concatenate([jnp.where(low, down, 0.0), jnp.where(low, 0.0, down)], axis=0)
    pair = jnp.concatenate(
        [
            jnp.concatenate([jnp.where(wide, leafs, 0.0), jnp.where(wide, 0.0, leafs)], axis=0),
            jnp.concatenate([down, none], axis=0),
            jnp.concatenate([none, down], axis=0),
        ],
        axis=1,
    )
    far = jnp.dot(pair.astype(BF16), reach[...], preferred_element_type=F32)
    for l in range(leaf_dev):
        out[l] = (near[l] + far[l * cols : (l + 1) * cols]).astype(BF16)
    everything(SUMS).wait_send()


def per_device(panels, basis, transfer, near_blocks, coupling, near_list):
    n = lax.axis_size("leaf")
    leaf_dev, cols, points = panels.shape
    rank = basis.shape[1]
    slots = near_list.shape[1]
    shifts = coupling.shape[1]
    half = rank // 2
    leaves = n * leaf_dev
    coupling = coupling.transpose(1, 0, 2).reshape(shifts, 2, half, 2 * rank)
    coupling = coupling.transpose(0, 2, 1, 3).reshape(shifts, rank, 2 * rank)
    plane = min(8, n)
    lines = n // plane
    teams = plane * leaf_dev // 8
    chunk = min(8 // leaf_dev, lines)
    kinds = [min(2 ** len(b), 3) for b in axis_bits(leaf_dev.bit_length() - 1, n.bit_length() - 1)]
    wider = kinds[1] * kinds[2] if kinds[0] > 2 else 0
    dma = pltpu.SemaphoreType.DMA
    return pl.pallas_call(
        functools.partial(kernel, n),
        out_shape=pltpu.VMEM(panels.shape, BF16),
        in_specs=[pl.BlockSpec(memory_space=pl.ANY)] * 6,
        out_specs=pl.BlockSpec(memory_space=pltpu.VMEM),
        scratch_shapes=[
            pltpu.VMEM((leaves, cols, points), BF16),
            pltpu.VMEM(basis.shape, BF16),
            pltpu.VMEM(transfer.shape, BF16),
            pltpu.VMEM(near_blocks.shape, BF16),
            pltpu.VMEM((shifts + 1, rank, 2 * rank), BF16),
            pltpu.SMEM(near_list.shape, jnp.int32),
            pltpu.SMEM((kinds[1] * kinds[2], leaf_dev * leaf_dev + 2), jnp.int32),
            pltpu.VMEM((max(2 * chunk * (2 * leaf_dev - 1), 8) * rank, 2 * rank), F32),
            pltpu.VMEM(
                (plane * (lines // chunk), chunk * leaf_dev * half, 2 * rank * leaf_dev), BF16
            ),
            pltpu.VMEM((lines // chunk, chunk * half, 2 * rank * teams), BF16),
            pltpu.VMEM((lines * (leaf_dev + 1) * half, 2 * cols), BF16),
            pltpu.VMEM((3 * leaf_dev * rank, points), BF16),
            pltpu.VMEM((plane // 2, cols + half, leaf_dev * rank), F32),
            pltpu.VMEM((plane // 2, cols + half, leaf_dev * rank), BF16),
            pltpu.VMEM((plane // 2, cols + half, leaf_dev * rank), BF16),
            pltpu.VMEM((plane // 2 - 1, cols + half, leaf_dev * rank), BF16),
            pltpu.VMEM((plane // 2 - 1, cols + half, leaf_dev * rank), BF16),
            pltpu.VMEM((leaf_dev, cols, points), F32),
            dma((6,)),
            dma((4 + wider,)),
            dma((10 + wider,)),
            dma((3,)),
            dma((3,)),
        ],
        compiler_params=pltpu.CompilerParams(
            collective_id=0, has_side_effects=True, vmem_limit_bytes=60 * 2**20
        ),
    )(panels, basis, transfer, near_blocks, coupling, near_list)


def solution(mesh):
    placed = (
        P("leaf", None, None),
        P("leaf", None, None),
        P("leaf", None, None),
        P("leaf", None, None, None),
        P(),
        P("leaf", None),
    )
    return jax.shard_map(
        per_device, mesh=mesh, in_specs=placed, out_specs=P("leaf", None, None), check_vma=False
    )
```
